32 devices in a mesh: chan: 16 (over z, y, core), wall: 2 (over x).
Axes of the slice: x: 2, y: 2, z: 4, core: 2. Of those that a mesh axis runs over, the one named last changes fastest.
Arguments:
- coords: float32 [3, 16, 2, 4096], P(None, 'chan', 'wall'), as said below
- masses: float32 [16, 2, 4096], P('chan', 'wall'), may hold values from 0.5 to 2
- counts: int32 [16, 2, 16], P('chan', 'wall'), may hold values from 64 to 256
- lists: int32 [16, 2, 5, 16, 2], P('chan', 'wall'), may hold values from 0 to 47, as said below
Outputs:
- density: float32 [16, 2, 4096], P('chan', 'wall')
The draws below stay inside these ranges and needn't reach their ends.
Inputs may be any that keep to these rules, and one draw needn't show every extreme that they name: `lists`: each row of 2 entries names different tiles; tile t of extended slab s is s * 16 + t, slab 0 the lower cross-wall neighbour, 1 the slab itself, 2 the upper neighbour. `coords`: channel components lie in [0, 1), cross-wall and depth components in [0, 8).
All inputs are finite; a program needn't handle non-finite values.
Results may differ from the reference program's by a relative error of at most 0.0003.
Values sent between devices are 32-bit elements; how exact they have to be, the bound alone decides.
A program may use at most 64 MiB of HBM per device.

```python
import math
import jax
import jax.numpy as jnp
from jax import lax

TILE = 256
TILE_DEV = 16
NB = 2
R = 4
CHAN_SLABS = 16
WALL_SLABS = 2
PART = 4096


def draw_coords(key, part):
    unit = jax.random.uniform(key, (3, CHAN_SLABS, WALL_SLABS, TILE_DEV * TILE), jnp.float32)
    extent = jnp.array([1.0, 2.0 * R, 2.0 * R], jnp.float32).reshape(3, 1, 1, 1)
    return (unit * extent * 0.9999).astype(jnp.float32)


def draw_lists(key, part):
    choices_count = 3 * TILE_DEV
    scores = jax.random.randint(key, (CHAN_SLABS, WALL_SLABS, R + 1, TILE_DEV, choices_count), 0, 1 << 20, dtype=jnp.int32)
    distinct = scores * choices_count + jnp.arange(choices_count, dtype=jnp.int32)
    return jnp.argsort(distinct, axis=-1)[..., :NB].astype(jnp.int32)


def with_ends(drawn, own_key, low, top_value):
    spot = [jax.random.randint(jax.random.fold_in(own_key, axis), (), 0, length) for axis, length in enumerate(drawn.shape)]
    main_axis = drawn.shape.index(max(drawn.shape))
    neighbour = spot[:main_axis] + [(spot[main_axis] + 1) % drawn.shape[main_axis]] + spot[main_axis + 1:]
    return drawn.at[tuple(spot)].set(low).at[tuple(neighbour)].set(top_value)


def level_of(stream_key, dims, cuts, smallest, top_value):
    gain, own = 1.0, jax.random.fold_in(stream_key, 6)
    for axis_at, shards_of in cuts:
        draws = jnp.exp(jax.random.uniform(jax.random.fold_in(own, axis_at), (shards_of,), jnp.float32, smallest / len(cuts), top_value / len(cuts)))
        gain = gain * jnp.repeat(draws, dims[axis_at] // shards_of).reshape([-1 if axis == axis_at else 1 for axis in range(len(dims))])
    return gain


def setup_inputs(seed: int = 0) -> dict:
    streams_of = jax.random.split(jax.random.key(seed), 5)
    coords = draw_coords(jax.random.fold_in(streams_of[4], 71), 0)
    masses = jnp.clip(jnp.exp(math.log(2.0) - 1.3862944 * jax.random.uniform(streams_of[1], (CHAN_SLABS, WALL_SLABS, PART), jnp.float32) ** level_of(streams_of[1], (CHAN_SLABS, WALL_SLABS, PART), ((0, 16), (1, 2)), -0.2, 0.2)), 0.5, 2.0)
    counts = with_ends(jax.random.randint(streams_of[2], (CHAN_SLABS, WALL_SLABS, TILE_DEV), TILE // 4, TILE + 1), jax.random.fold_in(streams_of[2], 1), TILE // 4, TILE).astype(jnp.int32)
    lists = draw_lists(jax.random.fold_in(streams_of[4], 71), 0)
    return dict(coords=coords, masses=masses, counts=counts, lists=lists)


def spline(scaled):
    return (jnp.maximum(2.0 - scaled, 0.0) ** 3 * 0.25 - jnp.maximum(1.0 - scaled, 0.0) ** 3) * (1.0 / math.pi)

def pair_block(own_block, partner, partner_rows, offset):
    tile_count = own_block.shape[1]
    tile_len = own_block.shape[2]
    list_len = partner_rows.shape[1]
    picked = jnp.take(partner, partner_rows.reshape(-1), axis=1).reshape(4, tile_count, list_len, tile_len)
    wall_lift = (partner_rows // tile_count - 1).astype(jnp.float32) * (2.0 * R)
    reach = float(R)

    def single_tile(inputs):
        own_tile, theirs, shift_y = inputs
        delta_x = own_tile[0][None, :, None] - (theirs[0][:, None, :] + offset)
        delta_y = own_tile[1][None, :, None] - (theirs[1][:, None, :] + shift_y[:, None, None])
        delta_z = own_tile[2][None, :, None] - theirs[2][:, None, :]
        distance = jnp.sqrt(delta_x * delta_x + delta_y * delta_y + delta_z * delta_z + 0.0001)
        weight = spline(distance / reach)
        gained = lax.optimization_barrier(jnp.sum(weight * theirs[3][:, None, :], axis=(0, 2)))
        handed = lax.optimization_barrier(jnp.sum(weight * own_tile[3][None, :, None], axis=1))
        return (gained, handed)
    gained, handed = lax.map(single_tile, (jnp.moveaxis(own_block, 1, 0), jnp.moveaxis(picked, 1, 0), wall_lift))
    onehot = (partner_rows.reshape(-1)[:, None] == jnp.arange(partner.shape[1], dtype=jnp.int32)[None, :]).astype(jnp.float32)
    returned = jnp.dot(onehot.T, handed.reshape(-1, tile_len), precision=lax.Precision.HIGHEST)
    return (gained, returned)

def reference(coords, masses, counts, lists):
    tile_count = counts.shape[2]
    tile_len = masses.shape[2] // tile_count
    slots = jnp.arange(tile_len, dtype=jnp.int32)
    filled = (slots[None, None, None, :] < counts[..., None]).astype(jnp.float32)
    weighted = masses.reshape(filled.shape) * filled
    packed = jnp.concatenate([coords.reshape(3, CHAN_SLABS, WALL_SLABS, tile_count, tile_len), weighted[None]], axis=0)
    padded = jnp.pad(packed, ((0, 0), (0, 0), (1, 1), (0, 0), (0, 0)))
    extended = jnp.concatenate([padded[:, :, 0:WALL_SLABS], padded[:, :, 1:WALL_SLABS + 1], padded[:, :, 2:]], axis=3)
    flat_own = jnp.moveaxis(packed.reshape(4, -1, tile_count, tile_len), 1, 0)
    density = jnp.zeros((CHAN_SLABS, WALL_SLABS, tile_count, tile_len), jnp.float32)
    returns = jnp.zeros((CHAN_SLABS, WALL_SLABS, 3 * tile_count, tile_len), jnp.float32)
    for step in range(R + 1):
        partner = jnp.roll(extended, -step, axis=1)
        flat_partner = jnp.moveaxis(partner.reshape(4, -1, 3 * tile_count, tile_len), 1, 0)
        flat_lists = lists[:, :, step].reshape(-1, tile_count, NB)

        def per_device(inputs, offset=float(step)):
            return pair_block(inputs[0], inputs[1], inputs[2], offset)
        gained, handed = lax.map(per_device, (flat_own, flat_partner, flat_lists))
        density = density + gained.reshape(CHAN_SLABS, WALL_SLABS, tile_count, tile_len)
        if step > 0:
            returns = returns + jnp.roll(handed.reshape(CHAN_SLABS, WALL_SLABS, 3 * tile_count, tile_len), step, axis=0)
    lower = returns[:, :, :tile_count]
    center = returns[:, :, tile_count:2 * tile_count]
    upper = returns[:, :, 2 * tile_count:]
    from_below = jnp.pad(upper, ((0, 0), (1, 0), (0, 0), (0, 0)))[:, :WALL_SLABS]
    from_above = jnp.pad(lower, ((0, 0), (0, 1), (0, 0), (0, 0)))[:, 1:]
    total = density + center + from_below + from_above
    return (total * filled / (NB * tile_len)).reshape(CHAN_SLABS, WALL_SLABS, -1)
```

```python
import functools
import math

import jax
import jax.numpy as jnp
from jax import lax
from jax.experimental import pallas as pl
from jax.experimental.pallas import tpu as pltpu
from jax.sharding import PartitionSpec as P

NB = 2
R = 4
LANES = 128
ROWS = 64
SHIFT = 6
PIECE = 32
MESH = pl.DeviceIdType.MESH


def wall_cases(wall, walls, flip):
    cases = []
    for s in range(3):
        other = wall + (1 - s if flip else s - 1)
        cases.append((s, other, jnp.logical_and(other >= 0, other < walls)))
    return cases


def gather_kernel(chans, walls, own_ref, ext_ref, send_sem, recv_sem, local_sem):
    chan = lax.axis_index("chan")
    wall = lax.axis_index("wall")
    valid = 1 + (wall > 0).astype(jnp.int32) + (wall < walls - 1).astype(jnp.int32)
    keep = pltpu.make_async_copy(own_ref, ext_ref.at[1], local_sem)
    keep.start()
    barrier = pltpu.get_barrier_semaphore()
    for s, other, there in wall_cases(wall, walls, False):
        @pl.when(there)
        def _(s=s, other=other):
            for k in range(R + 1):
                if k == 0 and s == 1:
                    continue
                pl.semaphore_signal(
                    barrier, inc=1, device_id=(lax.rem(chan + k, chans), other), device_id_type=MESH
                )
    pl.semaphore_wait(barrier, (R + 1) * valid - 1)

    def copy(k, s, other):
        return pltpu.make_async_remote_copy(
            src_ref=own_ref,
            dst_ref=ext_ref.at[k * 3 + s],
            send_sem=send_sem.at[k * 3 + s],
            recv_sem=recv_sem.at[k * 3 + s],
            device_id=(lax.rem(chan + chans - k, chans), other),
            device_id_type=MESH,
        )

    for k in range(R, -1, -1):
        for s, other, there in wall_cases(wall, walls, True):
            if k == 0 and s == 1:
                continue

            @pl.when(there)
            def _(k=k, s=s, other=other):
                copy(k, s, other).start()

    for k in range(R + 1):
        for s, other, there in wall_cases(wall, walls, False):
            if k == 0 and s == 1:
                continue

            @pl.when(there)
            def _(k=k, s=s, other=other):
                copy(k, s, other).wait_recv()

    for k in range(R + 1):
        for s, other, there in wall_cases(wall, walls, True):
            if k == 0 and s == 1:
                continue

            @pl.when(there)
            def _(k=k, s=s, other=other):
                copy(k, s, other).wait_send()
    keep.wait()


def gather(own, chans, walls):
    slots = (R + 1) * 3
    return pl.pallas_call(
        functools.partial(gather_kernel, chans, walls),
        out_shape=jax.ShapeDtypeStruct((slots,) + own.shape, own.dtype),
        in_specs=[pl.BlockSpec(memory_space=pltpu.VMEM)],
        out_specs=pl.BlockSpec(memory_space=pl.ANY),
        scratch_shapes=[
            pltpu.SemaphoreType.DMA((slots,)),
            pltpu.SemaphoreType.DMA((slots,)),
            pltpu.SemaphoreType.DMA,
        ],
        compiler_params=pltpu.CompilerParams(collective_id=0, has_side_effects=True),
    )(own)


def splits(v):
    first = v.astype(jnp.bfloat16).astype(jnp.float32)
    rest = v - first
    second = rest.astype(jnp.bfloat16).astype(jnp.float32)
    third = (rest - second).astype(jnp.bfloat16).astype(jnp.float32)
    return first, second, third


def halves(block, row):
    low = jnp.broadcast_to(block[row : row + 1], block.shape)
    high = jnp.broadcast_to(block[row + 4 : row + 5], block.shape)
    spot = lax.broadcasted_iota(jnp.int32, block.shape, 0)
    return low, high, jnp.where(spot < 4, low, high)


def pair_kernel(
    walls,
    lists_ref,
    counts_ref,
    own_ref,
    ext_ref,
    gained_ref,
    handed_ref,
    afeat,
    wcol,
    bfeat,
    brow,
    gacc,
    hands,
    used,
    blocks_ref,
    queues,
    items,
    sizes,
    sem,
):
    tiles, _, tile_len = own_ref.shape
    slots = ext_ref.shape[0] * 2
    list_len = lists_ref.shape[0] // ((R + 1) * tiles)
    wall = lax.axis_index("wall")
    turned = [
        jnp.transpose((ext_ref[:, half + 3, LANES:] > 0.0).astype(jnp.float32), (1, 0))
        for half in (0, 4)
    ]
    used[...] = jnp.concatenate([turned[0][:1]] + [turned[1][:7]], axis=0).astype(jnp.int32)
    fetch = pltpu.make_async_copy(used, blocks_ref, sem)
    fetch.start()
    spot = lax.broadcasted_iota(jnp.int32, (8, tile_len), 0)
    part = jnp.bitwise_and(spot, 3)
    quarter = 1.0 / R
    base = jnp.where(part == 0, -0.5, jnp.where(part == 3, 0.0, -float(R))) * quarter
    scale = jnp.where(part == 3, 1.0, quarter)

    def own_pair(i, carry):
        block = own_ref[2 * i], own_ref[2 * i + 1]
        block = jnp.concatenate(block, axis=0)
        _, _, s = halves(block, 3)
        place = jnp.where(part == 3, 0.0, block * scale + base)
        square = place * place
        pairsum = square + pltpu.roll(square, 1, 0)
        total = pairsum + pltpu.roll(pairsum, 2, 0)
        full = jnp.where(part == 3, total, place)
        one, two, three = splits(full)
        ones = jnp.where(part == 3, 1.0, 0.0)
        weight = s * s * s
        rest = jnp.zeros((LANES - 80, tile_len), jnp.float32)
        stack = jnp.concatenate(
            [one, one, two, two, one, three, ones, ones, ones, weight, rest], axis=0
        )
        turned = jnp.transpose(stack, (1, 0))
        lane = lax.broadcasted_iota(jnp.int32, turned.shape, 1)
        low = jnp.bitwise_and(lane, 4) == 0
        inside = lane < 72
        for half in range(2):
            t = 2 * i + half
            keep = low if half == 0 else jnp.logical_not(low)
            mine = jnp.where(jnp.logical_and(keep, inside), turned, 0.0)
            other = pltpu.roll(mine, 4 if half == 0 else LANES - 4, 1)
            afeat[half * tiles + t] = mine.astype(jnp.bfloat16)
            afeat[(1 - half) * tiles + t] = other.astype(jnp.bfloat16)
            wcol[t] = jnp.broadcast_to(
                turned[:, 72 + 4 * half : 73 + 4 * half], (tile_len, LANES)
            )
            gacc[t] = jnp.zeros((tile_len, LANES), jnp.float32)
        return carry

    lax.fori_loop(0, tiles // 2, own_pair, 0)
    hands[...] = jnp.zeros_like(hands)

    for k in range(R + 1):
        for slab in range(3):
            edge = wall + slab - 1
            shift = jnp.where(
                part == 0, k * quarter, jnp.where(part == 1, (slab - 1) * 2.0, 0.0)
            )

            def ext_pair(i, carry, k=k, slab=slab, shift=shift):
                at = (k * 3 + slab) * (tiles // 2) + i
                block = ext_ref[at]
                low, high, s = halves(block, 3)
                filled = s > 0.0
                place = block * scale + (base + shift)
                place = jnp.where(jnp.logical_and(part < 3, filled), place, 0.0)
                s = jnp.where(filled, s, 1.0)
                s2 = s * s
                square = place * place
                pairsum = square + pltpu.roll(square, 1, 0)
                total = pairsum + pltpu.roll(pairsum, 2, 0)
                tail = jnp.where(filled, s2 * (total + 0.0001 / (R * R)), 128.0)
                full = jnp.where(part == 3, s2, -2.0 * s2 * place)
                one, two, three = splits(full)
                first, second, third = splits(tail)
                stack = jnp.concatenate(
                    [one, two, one, two, three, one, first, second, third, jnp.zeros_like(one)],
                    axis=0,
                )
                bfeat[at] = stack.astype(jnp.bfloat16)
                for half, root in enumerate((low, high)):
                    root = jnp.where(root > 0.0, root, 1.0)
                    brow[at * 2 + half, :8] = 2.0 * root
                    brow[at * 2 + half, 8:] = 4.0 * root * root * root
                return carry

            @pl.when(jnp.logical_and(edge >= 0, edge < walls))
            def _(ext_pair=ext_pair):
                lax.fori_loop(0, tiles // 2, ext_pair, 0)

    fetch.wait()

    classes = 2 * (tile_len // ROWS)
    room = queues.shape[0] // classes
    low = jnp.where(wall == 0, tiles, 0)
    high = jnp.where(wall == walls - 1, 2 * tiles, 3 * tiles)
    for c in range(classes):
        sizes[c] = 0

    def enlist(t, carry):
        groups = lax.shift_right_logical(counts_ref[t] + (ROWS - 1), SHIFT)
        kind = groups * 2 - 2
        first, second = sizes[kind], sizes[kind + 1]
        base = kind * room
        high_bits = lax.shift_left(t, 16)
        for k in range(R + 1):
            for j in range(list_len):
                tile = lists_ref[(k * tiles + t) * list_len + j]
                at = k * 3 * tiles + tile
                real = jnp.logical_and(tile >= low, tile < high).astype(jnp.int32)
                wide = blocks_ref[jnp.bitwise_and(at, 1), lax.shift_right_logical(at, 1)]
                packed = at + high_bits
                queues[base + first] = packed
                queues[base + room + second] = packed
                both = jnp.bitwise_and(wide, real)
                second = second + both
                first = first + (real - both)
        sizes[kind] = first
        sizes[kind + 1] = second
        return carry

    lax.fori_loop(0, tiles, enlist, 0)
    nothing = (tiles << 16) + slots
    ends = [0]
    for c in reversed(range(classes)):
        size = sizes[c]
        start = ends[-1]

        def move(i, carry, c=c, start=start):
            for d in range(4):
                items[2 * start + 4 * i + d] = queues[c * room + 4 * i + d]
            return carry

        lax.fori_loop(0, lax.shift_right_logical(size + 3, 2), move, 0)
        items[2 * start + size] = nothing
        ends.append(start + lax.shift_right_logical(size + 1, 1))
    for d in range(4):
        items[2 * ends[-1] + d] = nothing

    def body(*accs):
        pieces = tile_len // PIECE
        for ref in accs:
            pltpu.matmul_pop(ref)

        def fields(m):
            packed = items[m]
            at = jnp.bitwise_and(packed, 65535)
            return at, lax.shift_right_logical(packed, 16)

        def push(m, q):
            at, _ = fields(m)
            rhs = jnp.concatenate(
                [
                    bfeat[lax.shift_right_logical(at, 1)],
                    jnp.zeros((256 - 80, tile_len), jnp.bfloat16),
                ],
                axis=0,
            )
            pltpu.matmul_push_rhs(rhs, staging_register=0, mxu_index=q)

        def feed(which, q, p):
            lhs = afeat[which, p * PIECE : (p + 1) * PIECE]
            lhs = jnp.concatenate([lhs, jnp.zeros((PIECE, 256 - LANES), jnp.bfloat16)], axis=1)
            pltpu.matmul_acc_lhs(
                accs[q * pieces + p], lhs, load_staged_rhs=0 if p == 0 else None
            )

        def which_of(m):
            at, t = fields(m)
            return jnp.bitwise_and(at, 1) * tiles + t

        def run(j, carry, groups, width):
            now = [fields(2 * j + q) for q in range(2)]
            then = [which_of(2 * j + 2 + q) for q in range(2)]
            rows = [
                [brow[at, r * 8 : r * 8 + 8, h * LANES : (h + 1) * LANES] for r in range(2) for h in range(width)]
                for at, _ in now
            ]
            sums = [[None] * width for _ in now]
            for p in range(groups * ROWS // PIECE):
                for q, (at, t) in enumerate(now):
                    u = pltpu.matmul_pop(accs[q * pieces + p])
                    feed(then[q], q, p)
                    if p == 0:
                        push(2 * j + 4 + q, q)
                    for r in range(0, PIECE, 8):
                        here = pl.ds(p * PIECE + r, 8)
                        aw = wcol[t, here, :]
                        total = None
                        for h in range(width):
                            v = u[r : r + 8, h * LANES : (h + 1) * LANES]
                            o = jnp.maximum(rows[q][h] - v * lax.rsqrt(v), 0.0)
                            w = jnp.minimum(o * o * o, rows[q][width + h] - (v * o) * 3.0)
                            total = w if total is None else total + w
                            back = w * aw
                            sums[q][h] = back if sums[q][h] is None else sums[q][h] + back
                        gacc[t, here, :] += total
            for q, (at, t) in enumerate(now):
                for h in range(width):
                    hands[at, :, h * LANES : (h + 1) * LANES] += sums[q][h]
            return carry

        for q in range(2):
            push(q, q)
        for q in range(2):
            for p in range(pieces):
                feed(which_of(q), q, p)
        for q in range(2):
            push(2 + q, q)
        for c in range(classes):
            kind = classes - 1 - c
            lax.fori_loop(
                ends[c],
                ends[c + 1],
                functools.partial(run, groups=kind // 2 + 1, width=1 + kind % 2),
                0,
            )
        for q in range(2):
            for p in range(pieces):
                feed(which_of(q), q, p)
        for ref in accs:
            pltpu.matmul_pop(ref)

    pl.run_scoped(
        body,
        *[pltpu.ACC(q)((PIECE, 256), jnp.float32) for q in range(2) for _ in range(tile_len // PIECE)],
    )
    for t in range(tiles):
        gained_ref[t] = jnp.sum(jnp.sum(
            jnp.transpose(gacc[t], (1, 0)).reshape(LANES // 8, 8, tile_len), axis=0
        ), axis=0)
    handed_ref[...] = jnp.sum(hands[:slots], axis=1)


def pairs(lists, counts, own, ext, walls):
    tiles, _, tile_len = own.shape
    smem = pl.BlockSpec(memory_space=pltpu.SMEM)
    vmem = pl.BlockSpec(memory_space=pltpu.VMEM)
    slots = ext.shape[0] * 2
    return pl.pallas_call(
        functools.partial(pair_kernel, walls),
        out_shape=(
            jax.ShapeDtypeStruct((tiles, tile_len), jnp.float32),
            jax.ShapeDtypeStruct((slots, tile_len), jnp.float32),
        ),
        in_specs=[smem, smem, vmem, vmem],
        out_specs=(vmem, vmem),
        scratch_shapes=[
            pltpu.VMEM((2 * tiles, tile_len, LANES), jnp.bfloat16),
            pltpu.VMEM((tiles + 1, tile_len, LANES), jnp.float32),
            pltpu.VMEM((slots // 2 + 1, 80, tile_len), jnp.bfloat16),
            pltpu.VMEM((slots + 1, 16, tile_len), jnp.float32),
            pltpu.VMEM((tiles + 1, tile_len, LANES), jnp.float32),
            pltpu.VMEM((slots + 1, 8, tile_len), jnp.float32),
            pltpu.VMEM((8, slots // 2), jnp.int32),
            pltpu.SMEM((8, slots // 2), jnp.int32),
            pltpu.SMEM((2 * (tile_len // ROWS) * (lists.shape[0] + 8),), jnp.int32),
            pltpu.SMEM((lists.shape[0] + 32,), jnp.int32),
            pltpu.SMEM((2 * (tile_len // ROWS),), jnp.int32),
            pltpu.SemaphoreType.DMA,
        ],
    )(lists, counts, own, ext)


def return_kernel(
    chans, walls, tiles, gained_ref, handed_ref, over_ref, out_ref, held, send_sem, recv_sem
):
    chan = lax.axis_index("chan")
    wall = lax.axis_index("wall")
    valid = 1 + (wall > 0).astype(jnp.int32) + (wall < walls - 1).astype(jnp.int32)
    barrier = pltpu.get_barrier_semaphore()
    for s, other, there in wall_cases(wall, walls, True):
        @pl.when(there)
        def _(s=s, other=other):
            for k in range(1, R + 1):
                pl.semaphore_signal(
                    barrier,
                    inc=1,
                    device_id=(lax.rem(chan + chans - k, chans), other),
                    device_id_type=MESH,
                )
    pl.semaphore_wait(barrier, R * valid)

    def copy(k, s, other):
        slot = (k - 1) * 3 + s
        return pltpu.make_async_remote_copy(
            src_ref=handed_ref.at[pl.ds((k * 3 + s) * tiles, tiles)],
            dst_ref=held.at[slot],
            send_sem=send_sem.at[slot],
            recv_sem=recv_sem.at[slot],
            device_id=(lax.rem(chan + k, chans), other),
            device_id_type=MESH,
        )

    for k in range(R, 0, -1):
        for s, other, there in wall_cases(wall, walls, False):
            @pl.when(there)
            def _(k=k, s=s, other=other):
                copy(k, s, other).start()

    out_ref[...] = gained_ref[...]
    for k in range(1, R + 1):
        for s, other, there in wall_cases(wall, walls, True):
            @pl.when(there)
            def _(k=k, s=s, other=other):
                copy(k, s, other).wait_recv()
                out_ref[...] += held[(k - 1) * 3 + s] * over_ref[...]

    for k in range(1, R + 1):
        for s, other, there in wall_cases(wall, walls, False):
            @pl.when(there)
            def _(k=k, s=s, other=other):
                copy(k, s, other).wait_send()


def hand_back(gained, handed, over, chans, walls):
    tiles, tile_len = gained.shape
    vmem = pl.BlockSpec(memory_space=pltpu.VMEM)
    return pl.pallas_call(
        functools.partial(return_kernel, chans, walls, tiles),
        out_shape=jax.ShapeDtypeStruct(gained.shape, gained.dtype),
        in_specs=[vmem, vmem, vmem],
        out_specs=vmem,
        scratch_shapes=[
            pltpu.VMEM((R * 3, tiles, tile_len), jnp.float32),
            pltpu.SemaphoreType.DMA((R * 3,)),
            pltpu.SemaphoreType.DMA((R * 3,)),
        ],
        compiler_params=pltpu.CompilerParams(collective_id=1, has_side_effects=True),
    )(gained, handed, over)


def on_device(chans, walls, coords, masses, counts, lists):
    tiles = counts.shape[2]
    tile_len = masses.shape[2] // tiles
    slots = jnp.arange(tile_len, dtype=jnp.int32)
    filled = (slots[None, :] < counts[0, 0][:, None]).astype(jnp.float32)
    weighted = masses.reshape(tiles, tile_len)
    root = jnp.exp(jnp.log(weighted) * (1.0 / 3.0))
    root = root - (root * root * root - weighted) / (3.0 * root * root)
    own = jnp.concatenate([coords.reshape(3, tiles, tile_len), (root * filled)[None]], axis=0)
    own = jnp.moveaxis(own, 0, 1)
    ext = gather(own.reshape(tiles // 2, 8, tile_len), chans, walls)
    gained, handed = pairs(
        lists.reshape(-1), counts.reshape(-1), own, ext.reshape(-1, 8, tile_len), walls
    )
    over = filled / weighted
    total = hand_back(gained, handed, over, chans, walls)
    scale = 1.0 / (4.0 * math.pi * NB * tile_len)
    return (total * filled * scale).reshape(1, 1, -1)


def solution(mesh):
    placed = (
        P(None, "chan", "wall", None),
        P("chan", "wall", None),
        P("chan", "wall", None),
        P("chan", "wall", None, None, None),
    )
    body = functools.partial(on_device, mesh.shape["chan"], mesh.shape["wall"])
    return jax.shard_map(
        body, mesh=mesh, in_specs=placed, out_specs=P("chan", "wall", None), check_vma=False
    )
```

```python
import functools
import math

import jax
import jax.numpy as jnp
from jax import lax
from jax.experimental import pallas as pl
from jax.experimental.pallas import tpu as pltpu
from jax.sharding import PartitionSpec as P

NB = 2
R = 4
LANES = 128
ROWS = 64
SHIFT = 6
PIECE = 32
MESH = pl.DeviceIdType.MESH


def wall_cases(wall, walls, flip):
    cases = []
    for s in range(3):
        other = wall + (1 - s if flip else s - 1)
        cases.append((s, other, jnp.logical_and(other >= 0, other < walls)))
    return cases


def gather_kernel(
    chans,
    walls,
    coords_ref,
    masses_ref,
    counts_ref,
    ext_ref,
    over_ref,
    own_ref,
    send_sem,
    recv_sem,
    pass_sem,
    local_sem,
):
    chan = lax.axis_index("chan")
    wall = lax.axis_index("wall")
    odd = lax.rem(chan, 2)
    twin = chan + 1 - 2 * odd
    valid = 1 + (wall > 0).astype(jnp.int32) + (wall < walls - 1).astype(jnp.int32)
    barrier = pltpu.get_barrier_semaphore()
    for s, other, there in wall_cases(wall, walls, False):
        @pl.when(there)
        def _(s=s, other=other):
            for k in (0, 2, 4):
                if k == 0 and s == 1:
                    continue
                pl.semaphore_signal(
                    barrier, inc=1, device_id=(lax.rem(chan + k, chans), other), device_id_type=MESH
                )
    pl.semaphore_signal(barrier, inc=1, device_id=(twin, wall), device_id_type=MESH)

    tiles, tile_len = over_ref.shape[1:]
    parts = tile_len // LANES
    height = tiles * parts

    def load(ref, base):
        return jnp.concatenate(
            [ref[pl.ds(base + h, tiles, stride=parts), :] for h in range(parts)], axis=1
        )

    spot = lax.broadcasted_iota(jnp.int32, (tiles, tile_len), 0)
    slot = lax.broadcasted_iota(jnp.int32, (tiles, tile_len), 1)
    limit = jnp.zeros((tiles, tile_len), jnp.int32)
    for t in range(tiles):
        limit = jnp.where(spot == t, counts_ref[t], limit)
    filled = slot < limit
    mass = load(masses_ref, 0)
    root = jnp.exp(jnp.log(mass) * (1.0 / 3.0))
    root = root - (root * root * root - mass) / (3.0 * root * root)
    over_ref[0] = jnp.where(filled, 1.0, 0.0)
    over_ref[1] = jnp.where(filled, 1.0 / mass, 0.0)
    fields = [load(coords_ref, i * height) for i in range(3)] + [jnp.where(filled, root, 0.0)]
    for i, field in enumerate(fields):
        for h in range(parts):
            own_ref[h, pl.ds(i, tiles, stride=4), :] = field[:, h * LANES : (h + 1) * LANES]

    pl.semaphore_wait(barrier, 3 * valid)

    def copy(k, s, other):
        return pltpu.make_async_remote_copy(
            src_ref=own_ref,
            dst_ref=ext_ref.at[k * 3 + s],
            send_sem=send_sem.at[k * 3 + s],
            recv_sem=recv_sem.at[k * 3 + s],
            device_id=(lax.rem(chan + chans - k, chans), other),
            device_id_type=MESH,
        )

    def relay(k, s, own=False):
        into = k - 1 + 2 * odd
        return pltpu.make_async_remote_copy(
            src_ref=own_ref if own else ext_ref.at[k * 3 + s],
            dst_ref=ext_ref.at[into * 3 + s],
            send_sem=pass_sem.at[into * 3 + s],
            recv_sem=recv_sem.at[into * 3 + s],
            device_id=(twin, wall),
            device_id_type=MESH,
        )

    def each(flip, ks, order, run):
        cases = wall_cases(wall, walls, flip)
        for s in order:
            _, other, there = cases[s]
            for k in ks:
                if k == 0 and s == 1:
                    continue

                @pl.when(there)
                def _(k=k, s=s, other=other):
                    run(k, s, other)

    each(True, (2, 4), (1, 0, 2), lambda k, s, other: copy(k, s, other).start())
    each(True, (0,), (0, 2), lambda k, s, other: copy(k, s, other).start())
    keep = pltpu.make_async_copy(own_ref, ext_ref.at[1], local_sem)
    keep.start()

    def forward(k, s, other):
        copy(k, s, other).wait_recv()
        relay(k, s).start()

    @pl.when(odd == 0)
    def _():
        each(False, (2, 4), (1, 0, 2), forward)
        each(False, (0,), (0, 2), lambda k, s, other: copy(k, s, other).wait_recv())

    @pl.when(odd == 1)
    def _():
        relay(0, 1, True).start()
        each(False, (2,), (1,), forward)
        each(False, (0, 2), (0, 2), forward)
        each(False, (4,), (1, 0, 2), lambda k, s, other: copy(k, s, other).wait_recv())

    each(False, (1, 3), (1, 0, 2), lambda k, s, other: copy(k, s, other).wait_recv())
    each(True, (0, 2, 4), (0, 1, 2), lambda k, s, other: copy(k, s, other).wait_send())

    @pl.when(odd == 0)
    def _():
        each(False, (2, 4), (0, 1, 2), lambda k, s, other: relay(k, s).wait_send())

    @pl.when(odd == 1)
    def _():
        relay(0, 1, True).wait_send()
        each(False, (0, 2), (0, 1, 2), lambda k, s, other: relay(k, s).wait_send())

    keep.wait()


def gather(coords, masses, counts, chans, walls):
    slots = (R + 1) * 3
    tiles = counts.shape[0]
    tile_len = masses.shape[0] * LANES // tiles
    vmem = pl.BlockSpec(memory_space=pltpu.VMEM)
    block = (tile_len // LANES, 4 * tiles, LANES)
    return pl.pallas_call(
        functools.partial(gather_kernel, chans, walls),
        out_shape=(
            jax.ShapeDtypeStruct((slots,) + block, jnp.float32),
            jax.ShapeDtypeStruct((2, tiles, tile_len), jnp.float32),
        ),
        in_specs=[vmem, vmem, pl.BlockSpec(memory_space=pltpu.SMEM)],
        out_specs=(pl.BlockSpec(memory_space=pl.ANY), vmem),
        scratch_shapes=[
            pltpu.VMEM(block, jnp.float32),
            pltpu.SemaphoreType.DMA((slots,)),
            pltpu.SemaphoreType.DMA((slots,)),
            pltpu.SemaphoreType.DMA((slots,)),
            pltpu.SemaphoreType.DMA,
        ],
        compiler_params=pltpu.CompilerParams(collective_id=0, has_side_effects=True),
    )(coords, masses, counts)


def splits(v):
    first = v.astype(jnp.bfloat16).astype(jnp.float32)
    rest = v - first
    second = rest.astype(jnp.bfloat16).astype(jnp.float32)
    third = (rest - second).astype(jnp.bfloat16).astype(jnp.float32)
    return first, second, third


def halves(block, row):
    low = jnp.broadcast_to(block[row : row + 1], block.shape)
    high = jnp.broadcast_to(block[row + 4 : row + 5], block.shape)
    spot = lax.broadcasted_iota(jnp.int32, block.shape, 0)
    return low, high, jnp.where(spot < 4, low, high)


def pair_kernel(
    walls,
    lists_ref,
    counts_ref,
    far_ref,
    gained_ref,
    handed_ref,
    afeat,
    wcol,
    bfeat,
    brow,
    gacc,
    hands,
    used,
    blocks_ref,
    queues,
    items,
    sizes,
    ext_ref,
    marks,
    sem,
    load_sem,
):
    tiles, tile_len = gained_ref.shape
    slots = handed_ref.shape[0]
    parts = tile_len // LANES
    list_len = lists_ref.shape[1]
    wall = lax.axis_index("wall")

    def bring(at):
        return pltpu.make_async_copy(far_ref.at[at], ext_ref.at[at], load_sem.at[at])

    def sides(run):
        for slab in range(3):
            edge = wall + slab - 1

            @pl.when(jnp.logical_and(edge >= 0, edge < walls))
            def _(slab=slab):
                for k in range(R + 1):
                    if k > 0 or slab != 1:
                        run(k * 3 + slab)

    bring(1).start()
    sides(lambda at: bring(at).start())
    bring(1).wait()

    def block_of(slab, i):
        rows = pl.ds(pl.multiple_of(i * 8, 8), 8)
        return jnp.concatenate([ext_ref[slab, h, rows, :] for h in range(parts)], axis=1)

    spot = lax.broadcasted_iota(jnp.int32, (8, tile_len), 0)
    part = jnp.bitwise_and(spot, 3)
    quarter = 1.0 / R
    base = jnp.where(part == 0, -0.5, jnp.where(part == 3, 0.0, -float(R))) * quarter
    scale = jnp.where(part == 3, 1.0, quarter)

    def own_pair(i, carry):
        block = block_of(1, i)
        _, _, s = halves(block, 3)
        place = jnp.where(part == 3, 0.0, block * scale + base)
        square = place * place
        pairsum = square + pltpu.roll(square, 1, 0)
        total = pairsum + pltpu.roll(pairsum, 2, 0)
        full = jnp.where(part == 3, total, place)
        one, two, three = splits(full)
        ones = jnp.where(part == 3, 1.0, 0.0)
        weight = s * s * s
        rest = jnp.zeros((LANES - 80, tile_len), jnp.float32)
        stack = jnp.concatenate(
            [one, one, two, two, one, three, ones, ones, ones, weight, rest], axis=0
        )
        turned = jnp.transpose(stack, (1, 0))
        lane = lax.broadcasted_iota(jnp.int32, turned.shape, 1)
        low = jnp.bitwise_and(lane, 4) == 0
        inside = lane < 72
        for half in range(2):
            t = 2 * i + half
            keep = low if half == 0 else jnp.logical_not(low)
            mine = jnp.where(jnp.logical_and(keep, inside), turned, 0.0)
            other = pltpu.roll(mine, 4 if half == 0 else LANES - 4, 1)
            afeat[half * tiles + t] = mine.astype(jnp.bfloat16)
            afeat[(1 - half) * tiles + t] = other.astype(jnp.bfloat16)
            wcol[t] = jnp.broadcast_to(
                turned[:, 72 + 4 * half : 73 + 4 * half], (tile_len, LANES)
            )
            gacc[t] = jnp.zeros((tile_len, LANES), jnp.float32)
        return carry

    lax.fori_loop(0, tiles // 2, own_pair, 0)
    sides(lambda at: bring(at).wait())
    for half in range(2):
        for at in range(ext_ref.shape[0]):
            marks[half, at * (tiles // 2) : (at + 1) * (tiles // 2), :] = ext_ref[
                at, 1, pl.ds(half * 4 + 3, tiles // 2, stride=8), :
            ]
    turned = [jnp.transpose((marks[half] > 0.0).astype(jnp.float32), (1, 0)) for half in range(2)]
    used[...] = jnp.concatenate([turned[0][:1], turned[1][:7]], axis=0).astype(jnp.int32)
    fetch = pltpu.make_async_copy(used, blocks_ref, sem)
    fetch.start()
    hands[...] = jnp.zeros_like(hands)

    for k in range(R + 1):
        for slab in range(3):
            edge = wall + slab - 1
            shift = jnp.where(
                part == 0, k * quarter, jnp.where(part == 1, (slab - 1) * 2.0, 0.0)
            )

            def ext_pair(i, carry, k=k, slab=slab, shift=shift):
                at = (k * 3 + slab) * (tiles // 2) + i
                block = block_of(k * 3 + slab, i)
                low, high, s = halves(block, 3)
                filled = s > 0.0
                place = block * scale + (base + shift)
                place = jnp.where(jnp.logical_and(part < 3, filled), place, 0.0)
                s = jnp.where(filled, s, 1.0)
                s2 = s * s
                square = place * place
                pairsum = square + pltpu.roll(square, 1, 0)
                total = pairsum + pltpu.roll(pairsum, 2, 0)
                tail = jnp.where(filled, s2 * (total + 0.0001 / (R * R)), 128.0)
                full = jnp.where(part == 3, s2, -2.0 * s2 * place)
                one, two, three = splits(full)
                first, second, third = splits(tail)
                stack = jnp.concatenate(
                    [one, two, one, two, three, one, first, second, third, jnp.zeros_like(one)],
                    axis=0,
                )
                bfeat[at] = stack.astype(jnp.bfloat16)
                for half, root in enumerate((low, high)):
                    root = jnp.where(root > 0.0, root, 1.0)
                    brow[at * 2 + half, :8] = 2.0 * root
                    brow[at * 2 + half, 8:] = 4.0 * root * root * root
                return carry

            @pl.when(jnp.logical_and(edge >= 0, edge < walls))
            def _(ext_pair=ext_pair):
                lax.fori_loop(0, tiles // 2, ext_pair, 0)

    fetch.wait()

    classes = 2 * (tile_len // ROWS)
    room = queues.shape[0] // classes
    low = jnp.where(wall == 0, tiles, 0)
    high = jnp.where(wall == walls - 1, 2 * tiles, 3 * tiles)
    for c in range(classes):
        sizes[c] = 0

    def enlist(t, carry):
        groups = lax.shift_right_logical(counts_ref[t] + (ROWS - 1), SHIFT)
        kind = groups * 2 - 2
        first, second = sizes[kind], sizes[kind + 1]
        base = kind * room
        high_bits = lax.shift_left(t, 16)
        for k in range(R + 1):
            for j in range(list_len):
                tile = lists_ref[k, j, t]
                at = k * 3 * tiles + tile
                real = jnp.logical_and(tile >= low, tile < high).astype(jnp.int32)
                wide = blocks_ref[jnp.bitwise_and(at, 1), lax.shift_right_logical(at, 1)]
                packed = at + high_bits
                queues[base + first] = packed
                queues[base + room + second] = packed
                both = jnp.bitwise_and(wide, real)
                second = second + both
                first = first + (real - both)
        sizes[kind] = first
        sizes[kind + 1] = second
        return carry

    lax.fori_loop(0, tiles, enlist, 0)
    nothing = (tiles << 16) + slots
    ends = [0]
    for c in reversed(range(classes)):
        size = sizes[c]
        start = ends[-1]

        def move(i, carry, c=c, start=start):
            for d in range(4):
                items[2 * start + 4 * i + d] = queues[c * room + 4 * i + d]
            return carry

        lax.fori_loop(0, lax.shift_right_logical(size + 3, 2), move, 0)
        items[2 * start + size] = nothing
        ends.append(start + lax.shift_right_logical(size + 1, 1))
    for d in range(4):
        items[2 * ends[-1] + d] = nothing

    def body(*accs):
        pieces = tile_len // PIECE
        for ref in accs:
            pltpu.matmul_pop(ref)

        def fields(m):
            packed = items[m]
            at = jnp.bitwise_and(packed, 65535)
            return at, lax.shift_right_logical(packed, 16)

        def push(m, q):
            at, _ = fields(m)
            rhs = jnp.concatenate(
                [
                    bfeat[lax.shift_right_logical(at, 1)],
                    jnp.zeros((256 - 80, tile_len), jnp.bfloat16),
                ],
                axis=0,
            )
            pltpu.matmul_push_rhs(rhs, staging_register=0, mxu_index=q)

        def feed(which, q, p):
            lhs = afeat[which, p * PIECE : (p + 1) * PIECE]
            lhs = jnp.concatenate([lhs, jnp.zeros((PIECE, 256 - LANES), jnp.bfloat16)], axis=1)
            pltpu.matmul_acc_lhs(
                accs[q * pieces + p], lhs, load_staged_rhs=0 if p == 0 else None
            )

        def which_of(m):
            at, t = fields(m)
            return jnp.bitwise_and(at, 1) * tiles + t

        def run(j, carry, groups, width):
            now = [fields(2 * j + q) for q in range(2)]
            then = [which_of(2 * j + 2 + q) for q in range(2)]
            rows = [
                [brow[at, r * 8 : r * 8 + 8, h * LANES : (h + 1) * LANES] for r in range(2) for h in range(width)]
                for at, _ in now
            ]
            sums = [[None] * width for _ in now]
            for p in range(groups * ROWS // PIECE):
                for q, (at, t) in enumerate(now):
                    u = pltpu.matmul_pop(accs[q * pieces + p])
                    feed(then[q], q, p)
                    if p == 0:
                        push(2 * j + 4 + q, q)
                    for r in range(0, PIECE, 8):
                        here = pl.ds(p * PIECE + r, 8)
                        aw = wcol[t, here, :]
                        total = None
                        for h in range(width):
                            v = u[r : r + 8, h * LANES : (h + 1) * LANES]
                            o = jnp.maximum(rows[q][h] - v * lax.rsqrt(v), 0.0)
                            w = jnp.minimum(o * o * o, rows[q][width + h] - (v * o) * 3.0)
                            total = w if total is None else total + w
                            back = w * aw
                            sums[q][h] = back if sums[q][h] is None else sums[q][h] + back
                        gacc[t, here, :] += total
            for q, (at, t) in enumerate(now):
                for h in range(width):
                    hands[at, :, h * LANES : (h + 1) * LANES] += sums[q][h]
            return carry

        for q in range(2):
            push(q, q)
        for q in range(2):
            for p in range(pieces):
                feed(which_of(q), q, p)
        for q in range(2):
            push(2 + q, q)
        for c in range(classes):
            kind = classes - 1 - c
            lax.fori_loop(
                ends[c],
                ends[c + 1],
                functools.partial(run, groups=kind // 2 + 1, width=1 + kind % 2),
                0,
            )
        for q in range(2):
            for p in range(pieces):
                feed(which_of(q), q, p)
        for ref in accs:
            pltpu.matmul_pop(ref)

    pl.run_scoped(
        body,
        *[pltpu.ACC(q)((PIECE, 256), jnp.float32) for q in range(2) for _ in range(tile_len // PIECE)],
    )
    for t in range(tiles):
        gained_ref[t] = jnp.sum(jnp.sum(
            jnp.transpose(gacc[t], (1, 0)).reshape(LANES // 8, 8, tile_len), axis=0
        ), axis=0)
    handed_ref[...] = jnp.sum(hands[:slots], axis=1)


def pairs(lists, counts, ext, walls):
    tiles = counts.shape[0]
    tile_len = ext.shape[1] * LANES
    smem = pl.BlockSpec(memory_space=pltpu.SMEM)
    vmem = pl.BlockSpec(memory_space=pltpu.VMEM)
    slots = ext.shape[0] * tiles
    entries = math.prod(lists.shape)
    return pl.pallas_call(
        functools.partial(pair_kernel, walls),
        out_shape=(
            jax.ShapeDtypeStruct((tiles, tile_len), jnp.float32),
            jax.ShapeDtypeStruct((slots, tile_len), jnp.float32),
        ),
        in_specs=[smem, smem, pl.BlockSpec(memory_space=pl.ANY)],
        out_specs=(vmem, vmem),
        scratch_shapes=[
            pltpu.VMEM((2 * tiles, tile_len, LANES), jnp.bfloat16),
            pltpu.VMEM((tiles + 1, tile_len, LANES), jnp.float32),
            pltpu.VMEM((slots // 2 + 1, 80, tile_len), jnp.bfloat16),
            pltpu.VMEM((slots + 1, 16, tile_len), jnp.float32),
            pltpu.VMEM((tiles + 1, tile_len, LANES), jnp.float32),
            pltpu.VMEM((slots + 1, 8, tile_len), jnp.float32),
            pltpu.VMEM((8, slots // 2), jnp.int32),
            pltpu.SMEM((8, slots // 2), jnp.int32),
            pltpu.SMEM((2 * (tile_len // ROWS) * (entries + 8),), jnp.int32),
            pltpu.SMEM((entries + 32,), jnp.int32),
            pltpu.SMEM((2 * (tile_len // ROWS),), jnp.int32),
            pltpu.VMEM(ext.shape, jnp.float32),
            pltpu.VMEM((2, slots // 2, LANES), jnp.float32),
            pltpu.SemaphoreType.DMA,
            pltpu.SemaphoreType.DMA((ext.shape[0],)),
        ],
    )(lists, counts, ext)


def return_kernel(
    chans, walls, tiles, gained_ref, handed_ref, over_ref, out_ref, held, hold, send_sem, recv_sem
):
    chan = lax.axis_index("chan")
    wall = lax.axis_index("wall")
    valid = 1 + (wall > 0).astype(jnp.int32) + (wall < walls - 1).astype(jnp.int32)
    barrier = pltpu.get_barrier_semaphore()
    for s, other, there in wall_cases(wall, walls, True):
        @pl.when(there)
        def _(s=s, other=other):
            for k in range(1, R + 1):
                pl.semaphore_signal(
                    barrier,
                    inc=1,
                    device_id=(lax.rem(chan + chans - k, chans), other),
                    device_id_type=MESH,
                )
    pl.semaphore_wait(barrier, R * valid)

    def copy(k, s, other):
        slot = (k - 1) * 3 + s
        return pltpu.make_async_remote_copy(
            src_ref=handed_ref.at[pl.ds((k * 3 + s) * tiles, tiles)],
            dst_ref=held.at[slot],
            send_sem=send_sem.at[slot],
            recv_sem=recv_sem.at[slot],
            device_id=(lax.rem(chan + k, chans), other),
            device_id_type=MESH,
        )

    for k in range(R, 0, -1):
        for s, other, there in wall_cases(wall, walls, False):
            @pl.when(there)
            def _(k=k, s=s, other=other):
                copy(k, s, other).start()

    total = gained_ref[...]
    scale = over_ref[0]
    back = over_ref[1]
    hold[...] = total * scale
    for k in range(1, R + 1):
        for s, other, there in wall_cases(wall, walls, True):
            @pl.when(there)
            def _(k=k, s=s, other=other):
                copy(k, s, other).wait_recv()
                hold[...] += held[(k - 1) * 3 + s] * back

    parts = hold.shape[1] // LANES
    for h in range(parts):
        out_ref[pl.ds(h, tiles, stride=parts), :] = hold[:, h * LANES : (h + 1) * LANES]
    for k in range(1, R + 1):
        for s, other, there in wall_cases(wall, walls, False):
            @pl.when(there)
            def _(k=k, s=s, other=other):
                copy(k, s, other).wait_send()


def hand_back(gained, handed, over, chans, walls):
    tiles, tile_len = gained.shape
    vmem = pl.BlockSpec(memory_space=pltpu.VMEM)
    return pl.pallas_call(
        functools.partial(return_kernel, chans, walls, tiles),
        out_shape=jax.ShapeDtypeStruct((tiles * tile_len // LANES, LANES), gained.dtype),
        in_specs=[vmem, vmem, vmem],
        out_specs=vmem,
        scratch_shapes=[
            pltpu.VMEM((R * 3, tiles, tile_len), jnp.float32),
            pltpu.VMEM((tiles, tile_len), jnp.float32),
            pltpu.SemaphoreType.DMA((R * 3,)),
            pltpu.SemaphoreType.DMA((R * 3,)),
        ],
        compiler_params=pltpu.CompilerParams(collective_id=1, has_side_effects=True),
    )(gained, handed, over)


def on_device(chans, walls, coords, masses, counts, lists):
    tiles = counts.shape[2]
    tile_len = masses.shape[2] // tiles
    scale = 1.0 / (4.0 * math.pi * NB * tile_len)
    counts = counts.reshape(-1)
    ext, over = gather(
        coords.reshape(-1, LANES), masses.reshape(-1, LANES), counts, chans, walls
    )
    lists = jnp.swapaxes(lists.reshape(lists.shape[2:]), 1, 2)
    gained, handed = pairs(lists, counts, ext, walls)
    total = hand_back(gained, handed, over, chans, walls)
    return total.reshape(1, 1, -1) * scale


def solution(mesh):
    placed = (
        P(None, "chan", "wall", None),
        P("chan", "wall", None),
        P("chan", "wall", None),
        P("chan", "wall", None, None, None),
    )
    body = functools.partial(on_device, mesh.shape["chan"], mesh.shape["wall"])
    return jax.shard_map(
        body, mesh=mesh, in_specs=placed, out_specs=P("chan", "wall", None), check_vma=False
    )
```

```python
import functools
import math

import jax
import jax.numpy as jnp
from jax import lax
from jax.experimental import pallas as pl
from jax.experimental.pallas import tpu as pltpu
from jax.sharding import PartitionSpec as P

NB = 2
R = 4
LANES = 128
ROWS = 64
SHIFT = 6
PIECE = 32
MESH = pl.DeviceIdType.MESH


def wall_cases(wall, walls):
    return [(0, wall - 1, wall > 0), (1, wall + 1, wall < walls - 1)]


def gather_kernel(
    chans,
    walls,
    coords_in,
    masses_in,
    tally_in,
    lists_in,
    ext_ref,
    over_out,
    sizes_ref,
    names_ref,
    coords_ref,
    masses_ref,
    tally_ref,
    lists_ref,
    over_ref,
    own_ref,
    send_sem,
    recv_sem,
    pass_sem,
    size_send,
    size_recv,
    name_send,
    name_recv,
    local_sem,
):
    chan = lax.axis_index("chan")
    wall = lax.axis_index("wall")
    odd = lax.rem(chan, 2)
    twin = chan + 1 - 2 * odd
    sides = (wall > 0).astype(jnp.int32) + (wall < walls - 1).astype(jnp.int32)
    fetches = [
        pltpu.make_async_copy(source, target, local_sem.at[i])
        for i, (source, target) in enumerate(
            (
                (masses_in, masses_ref),
                (tally_in, tally_ref),
                (coords_in, coords_ref),
                (lists_in, lists_ref),
            )
        )
    ]
    for one in fetches:
        one.start()
    barrier = pltpu.get_barrier_semaphore()
    for k in range(1, R + 1):
        target = (lax.rem(chan + k, chans), wall)
        pl.semaphore_signal(barrier, inc=1, device_id=target, device_id_type=MESH)

    @pl.when(odd == 1)
    def _():
        pl.semaphore_signal(barrier, inc=1, device_id=(twin, wall), device_id_type=MESH)

    for _, other, there in wall_cases(wall, walls):
        @pl.when(there)
        def _(other=other):
            pl.semaphore_signal(barrier, inc=1, device_id=(chan, other), device_id_type=MESH)

    tiles, tile_len = over_ref.shape[1:]
    parts = tile_len // LANES
    height = tiles * parts

    def load(ref, base):
        return jnp.concatenate(
            [ref[pl.ds(base + h, tiles, stride=parts), :] for h in range(parts)], axis=1
        )

    spot = lax.broadcasted_iota(jnp.int32, (tiles, tile_len), 0)
    slot = lax.broadcasted_iota(jnp.int32, (tiles, tile_len), 1)
    for one in fetches:
        one.wait()
    tally = jnp.broadcast_to(tally_ref[...].astype(jnp.float32), (tiles, tiles))
    same = spot[:, :tiles] == slot[:, :tiles]
    limit = jnp.sum(jnp.where(same, tally, 0.0), axis=1, keepdims=True)
    filled = slot.astype(jnp.float32) < limit
    mass = load(masses_ref, 0)
    root = jnp.exp(jnp.log(mass) * (1.0 / 3.0))
    root = root - (root * root * root - mass) / (3.0 * root * root)
    over_ref[0] = jnp.where(filled, 1.0, 0.0)
    over_ref[1] = jnp.where(filled, 1.0 / mass, 0.0)
    fields = [load(coords_ref, i * height) for i in range(3)] + [jnp.where(filled, root, 0.0)]
    for i, field in enumerate(fields):
        for h in range(parts):
            own_ref[h, pl.ds(i, tiles, stride=4), :] = field[:, h * LANES : (h + 1) * LANES]

    keep = [
        pltpu.make_async_copy(own_ref, ext_ref.at[0], local_sem.at[0]),
        pltpu.make_async_copy(tally_ref, sizes_ref.at[0], local_sem.at[1]),
        pltpu.make_async_copy(over_ref, over_out, local_sem.at[2]),
    ]
    pl.semaphore_wait(barrier, R + 1 + sides - odd)

    def remote(source, target, sent, got, device):
        return pltpu.make_async_remote_copy(
            src_ref=source,
            dst_ref=target,
            send_sem=sent,
            recv_sem=got,
            device_id=device,
            device_id_type=MESH,
        )

    def behind(k):
        return (lax.rem(chan + chans - k, chans), wall)

    def copy(k):
        return remote(own_ref, ext_ref.at[k], send_sem.at[k], recv_sem.at[k], behind(k))

    def tell(k):
        return remote(tally_ref, sizes_ref.at[k], size_send.at[k], size_recv.at[k], behind(k))

    def aside(side, other):
        slab = R + 1 + side
        device = (chan, other)
        return (
            remote(own_ref, ext_ref.at[slab], send_sem.at[slab], recv_sem.at[slab], device),
            remote(
                tally_ref, sizes_ref.at[slab], size_send.at[slab], size_recv.at[slab], device
            ),
            remote(lists_ref, names_ref.at[side], name_send.at[side], name_recv.at[side], device),
        )

    def relay(k, own=False):
        into = k - 1 + 2 * odd
        source = own_ref if own else ext_ref.at[k]
        return remote(source, ext_ref.at[into], pass_sem.at[into], recv_sem.at[into], (twin, wall))

    copy(2).start()
    copy(4).start()
    for side, other, there in wall_cases(wall, walls):
        @pl.when(there)
        def _(side=side, other=other):
            for one in aside(1 - side, other):
                one.start()

    @pl.when(odd == 1)
    def _():
        relay(0, True).start()

    for k in range(1, R + 1):
        tell(k).start()
    for one in keep:
        one.start()

    @pl.when(odd == 0)
    def _():
        for k in (2, 4):
            copy(k).wait_recv()
            relay(k).start()

    @pl.when(odd == 1)
    def _():
        copy(2).wait_recv()
        relay(2).start()
        copy(4).wait_recv()

    for k in range(1, R + 1):
        tell(k).wait()
    for side, other, there in wall_cases(wall, walls):
        @pl.when(there)
        def _(side=side, other=other):
            for one in aside(side, other):
                one.wait_recv()
            for one in aside(1 - side, other):
                one.wait_send()

    copy(1).wait_recv()
    copy(3).wait_recv()
    copy(2).wait_send()
    copy(4).wait_send()

    @pl.when(odd == 0)
    def _():
        relay(2).wait_send()
        relay(4).wait_send()

    @pl.when(odd == 1)
    def _():
        relay(0, True).wait_send()
        relay(2).wait_send()

    for one in keep:
        one.wait()


def gather(coords, masses, counts, lists, chans, walls):
    slabs = R + 3
    tiles = counts.shape[0]
    tile_len = masses.shape[0] * LANES // tiles
    hbm = pl.BlockSpec(memory_space=pl.ANY)
    block = (tile_len // LANES, 4 * tiles, LANES)
    tally = counts.reshape(1, tiles)
    many = pltpu.SemaphoreType.DMA((slabs,))
    few = pltpu.SemaphoreType.DMA((2,))
    return pl.pallas_call(
        functools.partial(gather_kernel, chans, walls),
        out_shape=(
            jax.ShapeDtypeStruct((slabs,) + block, jnp.float32),
            jax.ShapeDtypeStruct((2, tiles, tile_len), jnp.float32),
            jax.ShapeDtypeStruct((slabs,) + tally.shape, jnp.int32),
            jax.ShapeDtypeStruct((2,) + lists.shape, jnp.int32),
        ),
        in_specs=[hbm] * 4,
        out_specs=(hbm,) * 4,
        scratch_shapes=[
            pltpu.VMEM(coords.shape, jnp.float32),
            pltpu.VMEM(masses.shape, jnp.float32),
            pltpu.VMEM(tally.shape, jnp.int32),
            pltpu.VMEM(lists.shape, jnp.int32),
            pltpu.VMEM((2, tiles, tile_len), jnp.float32),
            pltpu.VMEM(block, jnp.float32),
            many,
            many,
            many,
            many,
            many,
            few,
            few,
            pltpu.SemaphoreType.DMA((4,)),
        ],
        compiler_params=pltpu.CompilerParams(collective_id=0, has_side_effects=True),
    )(coords, masses, tally, lists)


def splits(v):
    first = v.astype(jnp.bfloat16).astype(jnp.float32)
    rest = v - first
    second = rest.astype(jnp.bfloat16).astype(jnp.float32)
    third = (rest - second).astype(jnp.bfloat16).astype(jnp.float32)
    return first, second, third


def halves(block, row):
    low = jnp.broadcast_to(block[row : row + 1], block.shape)
    high = jnp.broadcast_to(block[row + 4 : row + 5], block.shape)
    spot = lax.broadcasted_iota(jnp.int32, block.shape, 0)
    return low, high, jnp.where(spot < 4, low, high)


def pair_kernel(
    walls,
    lists_ref,
    names_ref,
    counts_ref,
    far_ref,
    gained_ref,
    handed_ref,
    afeat,
    wcol,
    bfeat,
    brow,
    gacc,
    hands,
    queues,
    items,
    sizes,
    ext_ref,
    load_sem,
):
    _, tiles, tile_len = gained_ref.shape
    slots = (R + 1) * tiles
    parts = tile_len // LANES
    list_len = lists_ref.shape[1]
    wall = lax.axis_index("wall")
    near = ((0, wall > 0), (1, wall < walls - 1))
    slabs = far_ref.shape[0]

    def bring(at):
        return pltpu.make_async_copy(far_ref.at[at], ext_ref.at[at], load_sem.at[at])

    bring(0).start()
    for side, there in near:
        pl.when(there)(lambda side=side: bring(R + 1 + side).start())
    for k in range(1, R + 1):
        bring(k).start()
    classes = 2 * (tile_len // ROWS)
    room = queues.shape[0] // classes
    for c in range(classes):
        sizes[c] = 0

    def block_of(slab, i):
        rows = pl.ds(pl.multiple_of(i * 8, 8), 8)
        return jnp.concatenate([ext_ref[slab, h, rows, :] for h in range(parts)], axis=1)

    spot = lax.broadcasted_iota(jnp.int32, (8, tile_len), 0)
    part = jnp.bitwise_and(spot, 3)
    quarter = 1.0 / R
    base = jnp.where(part == 0, -0.5, jnp.where(part == 3, 0.0, -float(R))) * quarter
    scale = jnp.where(part == 3, 1.0, quarter)

    def own_pair(i, a):
        block = block_of((0, R + 1, R + 2)[a], i)
        _, _, s = halves(block, 3)
        lift = jnp.where(part == 1, (0.0, -2.0, 2.0)[a], 0.0)
        place = jnp.where(part == 3, 0.0, block * scale + (base + lift))
        square = place * place
        pairsum = square + pltpu.roll(square, 1, 0)
        total = pairsum + pltpu.roll(pairsum, 2, 0)
        full = jnp.where(part == 3, total, place)
        one, two, three = splits(full)
        ones = jnp.where(part == 3, 1.0, 0.0)
        weight = s * s * s
        rest = jnp.zeros((LANES - 80, tile_len), jnp.float32)
        stack = jnp.concatenate(
            [one, one, two, two, one, three, ones, ones, ones, weight, rest], axis=0
        )
        turned = jnp.transpose(stack, (1, 0))
        lane = lax.broadcasted_iota(jnp.int32, turned.shape, 1)
        low = jnp.bitwise_and(lane, 4) == 0
        inside = lane < 72
        for half in range(2):
            t = 2 * i + half + a * tiles
            keep = low if half == 0 else jnp.logical_not(low)
            mine = jnp.where(jnp.logical_and(keep, inside), turned, 0.0)
            other = pltpu.roll(mine, 4 if half == 0 else LANES - 4, 1)
            afeat[half * 3 * tiles + t] = mine.astype(jnp.bfloat16)
            afeat[(1 - half) * 3 * tiles + t] = other.astype(jnp.bfloat16)
            wcol[t] = jnp.broadcast_to(
                turned[:, 72 + 4 * half : 73 + 4 * half], (tile_len, LANES)
            )
            gacc[t] = jnp.zeros((tile_len, LANES), jnp.float32)

    def enlist(t, a):
        groups = lax.shift_right_logical(
            counts_ref[(0, R + 1, R + 2)[a], 0, t] + (ROWS - 1), SHIFT
        )
        kind = groups * 2 - 2
        first, second = sizes[kind], sizes[kind + 1]
        base = kind * room
        high_bits = lax.shift_left(t + a * tiles, 16)
        low = (1, 2, 0)[a] * tiles
        for k in range(R + 1):
            for j in range(list_len):
                tile = lists_ref[k, j, t] if a == 0 else names_ref[a - 1, k, j, t]
                inside = jnp.logical_and(tile >= low, tile < low + tiles)
                at = jnp.where(inside, tile - low, 0)
                real = inside.astype(jnp.int32)
                wide = (counts_ref[k, 0, at] > LANES).astype(jnp.int32)
                packed = at + (high_bits + k * tiles)
                queues[base + first] = packed
                queues[base + room + second] = packed
                both = jnp.bitwise_and(wide, real)
                second = second + both
                first = first + (real - both)
        sizes[kind] = first
        sizes[kind + 1] = second

    def prepare(a):
        bring((0, R + 1, R + 2)[a]).wait()

        def pair_of(i, carry):
            enlist(2 * i, a)
            enlist(2 * i + 1, a)
            own_pair(i, a)
            return carry

        lax.fori_loop(0, tiles // 2, pair_of, 0)

    prepare(0)
    hands[...] = jnp.zeros_like(hands)
    for side, there in near:
        pl.when(there)(functools.partial(prepare, side + 1))
    for k in range(1, R + 1):
        bring(k).wait()

    def ext_pair(i, k):
        at = k * (tiles // 2) + i
        block = block_of(k, i)
        low, high, s = halves(block, 3)
        filled = s > 0.0
        place = block * scale + (base + jnp.where(part == 0, k * quarter, 0.0))
        place = jnp.where(jnp.logical_and(part < 3, filled), place, 0.0)
        s = jnp.where(filled, s, 1.0)
        s2 = s * s
        square = place * place
        pairsum = square + pltpu.roll(square, 1, 0)
        total = pairsum + pltpu.roll(pairsum, 2, 0)
        tail = jnp.where(filled, s2 * (total + 0.0001 / (R * R)), 128.0)
        full = jnp.where(part == 3, s2, -2.0 * s2 * place)
        one, two, three = splits(full)
        first, second, third = splits(tail)
        stack = jnp.concatenate(
            [one, two, one, two, three, one, first, second, third, jnp.zeros_like(one)],
            axis=0,
        )
        bfeat[at] = stack.astype(jnp.bfloat16)
        for half, root in enumerate((low, high)):
            root = jnp.where(root > 0.0, root, 1.0)
            brow[at * 2 + half, :8] = 2.0 * root
            brow[at * 2 + half, 8:] = 4.0 * root * root * root

    def ext_pairs(i, carry):
        for k in range(R + 1):
            ext_pair(i, k)
        return carry

    lax.fori_loop(0, tiles // 2, ext_pairs, 0)
    nothing = ((3 * tiles) << 16) + slots
    ends = [0]
    for c in reversed(range(classes)):
        size = sizes[c]
        start = ends[-1]

        def move(i, carry, c=c, start=start):
            for d in range(4):
                items[2 * start + 4 * i + d] = queues[c * room + 4 * i + d]
            return carry

        lax.fori_loop(0, lax.shift_right_logical(size + 3, 2), move, 0)
        items[2 * start + size] = nothing
        ends.append(start + lax.shift_right_logical(size + 1, 1))
    for d in range(4):
        items[2 * ends[-1] + d] = nothing

    def body(*accs):
        pieces = tile_len // PIECE
        for ref in accs:
            pltpu.matmul_pop(ref)

        def fields(m):
            packed = items[m]
            at = jnp.bitwise_and(packed, 65535)
            return at, lax.shift_right_logical(packed, 16)

        def push(m, q):
            at, _ = fields(m)
            rhs = jnp.concatenate(
                [
                    bfeat[lax.shift_right_logical(at, 1)],
                    jnp.zeros((256 - 80, tile_len), jnp.bfloat16),
                ],
                axis=0,
            )
            pltpu.matmul_push_rhs(rhs, staging_register=0, mxu_index=q)

        def feed(which, q, p):
            lhs = afeat[which, p * PIECE : (p + 1) * PIECE]
            lhs = jnp.concatenate([lhs, jnp.zeros((PIECE, 256 - LANES), jnp.bfloat16)], axis=1)
            pltpu.matmul_acc_lhs(
                accs[q * pieces + p], lhs, load_staged_rhs=0 if p == 0 else None
            )

        def which_of(m):
            at, t = fields(m)
            return jnp.bitwise_and(at, 1) * (3 * tiles) + t

        def run(j, carry, groups, width):
            now = [fields(2 * j + q) for q in range(2)]
            then = [which_of(2 * j + 2 + q) for q in range(2)]
            rows = [
                [brow[at, r * 8 : r * 8 + 8, h * LANES : (h + 1) * LANES] for r in range(2) for h in range(width)]
                for at, _ in now
            ]
            sums = [[None] * width for _ in now]
            for p in range(groups * ROWS // PIECE):
                for q, (at, t) in enumerate(now):
                    u = pltpu.matmul_pop(accs[q * pieces + p])
                    feed(then[q], q, p)
                    if p == 0:
                        push(2 * j + 4 + q, q)
                    for r in range(0, PIECE, 8):
                        here = pl.ds(p * PIECE + r, 8)
                        aw = wcol[t, here, :]
                        total = None
                        for h in range(width):
                            v = u[r : r + 8, h * LANES : (h + 1) * LANES]
                            o = jnp.maximum(rows[q][h] - v * lax.rsqrt(v), 0.0)
                            w = jnp.minimum(o * o * o, rows[q][width + h] - (v * o) * 3.0)
                            total = w if total is None else total + w
                            back = w * aw
                            sums[q][h] = back if sums[q][h] is None else sums[q][h] + back
                        gacc[t, here, :] += total
            for q, (at, t) in enumerate(now):
                for h in range(width):
                    hands[at, :, h * LANES : (h + 1) * LANES] += sums[q][h]
            return carry

        for q in range(2):
            push(q, q)
        for q in range(2):
            for p in range(pieces):
                feed(which_of(q), q, p)
        for q in range(2):
            push(2 + q, q)
        for c in range(classes):
            kind = classes - 1 - c
            lax.fori_loop(
                ends[c],
                ends[c + 1],
                functools.partial(run, groups=kind // 2 + 1, width=1 + kind % 2),
                0,
            )
        for q in range(2):
            for p in range(pieces):
                feed(which_of(q), q, p)
        for ref in accs:
            pltpu.matmul_pop(ref)

    pl.run_scoped(
        body,
        *[pltpu.ACC(q)((PIECE, 256), jnp.float32) for q in range(2) for _ in range(tile_len // PIECE)],
    )
    lane = lax.broadcasted_iota(jnp.int32, (tile_len, LANES), 1)

    def finish(a):
        columns = jnp.zeros((tile_len, LANES), jnp.float32)
        for t in range(tiles):
            value = jnp.sum(gacc[a * tiles + t], axis=1, keepdims=True)
            columns = jnp.where(lane == t, value, columns)
        gained_ref[a] = jnp.transpose(columns, (1, 0))[:tiles]

    finish(0)
    for side, there in near:
        pl.when(there)(functools.partial(finish, side + 1))
    handed_ref[...] = jnp.sum(hands[tiles:slots], axis=1).reshape(handed_ref.shape)


def pairs(lists, names, counts, ext, walls):
    tiles = counts.shape[2]
    tile_len = ext.shape[1] * LANES
    smem = pl.BlockSpec(memory_space=pltpu.SMEM)
    vmem = pl.BlockSpec(memory_space=pltpu.VMEM)
    slots = (R + 1) * tiles
    entries = 3 * math.prod(lists.shape)
    return pl.pallas_call(
        functools.partial(pair_kernel, walls),
        out_shape=(
            jax.ShapeDtypeStruct((3, tiles, tile_len), jnp.float32),
            jax.ShapeDtypeStruct((R, tiles, tile_len), jnp.float32),
        ),
        in_specs=[smem, smem, smem, pl.BlockSpec(memory_space=pl.ANY)],
        out_specs=(vmem, vmem),
        scratch_shapes=[
            pltpu.VMEM((6 * tiles, tile_len, LANES), jnp.bfloat16),
            pltpu.VMEM((3 * tiles + 1, tile_len, LANES), jnp.float32),
            pltpu.VMEM((slots // 2 + 1, 80, tile_len), jnp.bfloat16),
            pltpu.VMEM((slots + 1, 16, tile_len), jnp.float32),
            pltpu.VMEM((3 * tiles + 1, tile_len, LANES), jnp.float32),
            pltpu.VMEM((slots + 1, 8, tile_len), jnp.float32),
            pltpu.SMEM((2 * (tile_len // ROWS) * (entries + 8),), jnp.int32),
            pltpu.SMEM((entries + 32,), jnp.int32),
            pltpu.SMEM((2 * (tile_len // ROWS),), jnp.int32),
            pltpu.VMEM(ext.shape, jnp.float32),
            pltpu.SemaphoreType.DMA((ext.shape[0],)),
        ],
    )(lists, names, counts, ext)


def return_kernel(
    chans,
    walls,
    gained_in,
    handed_in,
    over_in,
    out_ref,
    gained_ref,
    handed_ref,
    over_ref,
    held,
    hold,
    send_sem,
    recv_sem,
    local_sem,
):
    chan = lax.axis_index("chan")
    wall = lax.axis_index("wall")
    sides = (wall > 0).astype(jnp.int32) + (wall < walls - 1).astype(jnp.int32)
    pulls = [
        pltpu.make_async_copy(source, target, local_sem.at[i])
        for i, (source, target) in enumerate(
            ((handed_in, handed_ref), (gained_in, gained_ref), (over_in, over_ref))
        )
    ]
    for one in pulls:
        one.start()
    barrier = pltpu.get_barrier_semaphore()
    for k in range(1, R + 1):
        target = (lax.rem(chan + chans - k, chans), wall)
        pl.semaphore_signal(barrier, inc=1, device_id=target, device_id_type=MESH)
    for _, other, there in wall_cases(wall, walls):
        @pl.when(there)
        def _(other=other):
            pl.semaphore_signal(barrier, inc=1, device_id=(chan, other), device_id_type=MESH)
    for one in pulls:
        one.wait()
    pl.semaphore_wait(barrier, R + sides)

    def copy(source, slot, device):
        return pltpu.make_async_remote_copy(
            src_ref=source,
            dst_ref=held.at[slot],
            send_sem=send_sem.at[slot],
            recv_sem=recv_sem.at[slot],
            device_id=device,
            device_id_type=MESH,
        )

    def ahead(k):
        return copy(handed_ref.at[k - 1], k - 1, (lax.rem(chan + k, chans), wall))

    def aside(side, slot, other):
        return copy(gained_ref.at[side + 1], R + slot, (chan, other))

    for k in range(R, 0, -1):
        ahead(k).start()
    for side, other, there in wall_cases(wall, walls):
        @pl.when(there)
        def _(side=side, other=other):
            aside(side, 1 - side, other).start()

    tiles = hold.shape[0]
    hold[...] = gained_ref[0]
    for side, other, there in wall_cases(wall, walls):
        @pl.when(there)
        def _(side=side, other=other):
            aside(side, side, other).wait_recv()
            hold[...] += held[R + side]

    handed = None
    for k in range(1, R + 1):
        ahead(k).wait_recv()
        handed = held[k - 1] if handed is None else handed + held[k - 1]
    total = hold[...] * over_ref[0] + handed * over_ref[1]
    parts = hold.shape[1] // LANES
    for h in range(parts):
        out_ref[pl.ds(h, tiles, stride=parts), :] = total[:, h * LANES : (h + 1) * LANES]
    for k in range(1, R + 1):
        ahead(k).wait_send()
    for side, other, there in wall_cases(wall, walls):
        @pl.when(there)
        def _(side=side, other=other):
            aside(side, 1 - side, other).wait_send()


def hand_back(gained, handed, over, chans, walls):
    _, tiles, tile_len = gained.shape
    vmem = pl.BlockSpec(memory_space=pltpu.VMEM)
    return pl.pallas_call(
        functools.partial(return_kernel, chans, walls),
        out_shape=jax.ShapeDtypeStruct((tiles * tile_len // LANES, LANES), gained.dtype),
        in_specs=[pl.BlockSpec(memory_space=pl.ANY)] * 3,
        out_specs=vmem,
        scratch_shapes=[
            pltpu.VMEM(gained.shape, jnp.float32),
            pltpu.VMEM(handed.shape, jnp.float32),
            pltpu.VMEM(over.shape, jnp.float32),
            pltpu.VMEM((R + 2, tiles, tile_len), jnp.float32),
            pltpu.VMEM((tiles, tile_len), jnp.float32),
            pltpu.SemaphoreType.DMA((R + 2,)),
            pltpu.SemaphoreType.DMA((R + 2,)),
            pltpu.SemaphoreType.DMA((3,)),
        ],
        compiler_params=pltpu.CompilerParams(collective_id=1, has_side_effects=True),
    )(gained, handed, over)


def on_device(chans, walls, coords, masses, counts, lists):
    tiles = counts.shape[2]
    tile_len = masses.shape[2] // tiles
    scale = 1.0 / (4.0 * math.pi * NB * tile_len)
    lists = jnp.swapaxes(lists.reshape(lists.shape[2:]), 1, 2)
    ext, over, sizes, names = gather(
        coords.reshape(-1, LANES),
        masses.reshape(-1, LANES),
        counts.reshape(-1),
        lists,
        chans,
        walls,
    )
    gained, handed = pairs(lists, names, sizes, ext, walls)
    total = hand_back(gained, handed, over, chans, walls)
    return total.reshape(1, 1, -1) * scale


def solution(mesh):
    placed = (
        P(None, "chan", "wall", None),
        P("chan", "wall", None),
        P("chan", "wall", None),
        P("chan", "wall", None, None, None),
    )
    body = functools.partial(on_device, mesh.shape["chan"], mesh.shape["wall"])
    return jax.shard_map(
        body, mesh=mesh, in_specs=placed, out_specs=P("chan", "wall", None), check_vma=False
    )
```

```python
import functools
import math

import jax
import jax.numpy as jnp
from jax import lax
from jax.experimental import pallas as pl
from jax.experimental.pallas import tpu as pltpu
from jax.sharding import PartitionSpec as P

NB = 2
R = 4
LANES = 128
ROWS = 32
SHIFT = 5
PIECE = 32
MESH = pl.DeviceIdType.MESH


def wall_cases(wall, walls):
    return [(0, wall - 1, wall > 0), (1, wall + 1, wall < walls - 1)]


def arrange(
    wall, walls, tiles, tile_len, lists_ref, names_ref, tally_ref, sizes_ref, grid_ref, codes_ref
):
    list_len = lists_ref.shape[1]
    lines = codes_ref.shape[0]
    used = (R + 1) * list_len
    top = tile_len // ROWS
    shape = (lines, LANES)
    grid_ref[...] = jnp.zeros_like(grid_ref)
    for k in range(R + 1):
        rows = pl.ds(k * list_len, list_len)
        counts = tally_ref[...] if k == 0 else sizes_ref[k]
        grid_ref[3, rows, :tiles] = jnp.broadcast_to(counts, (list_len, tiles))
        for a in range(3):
            grid_ref[a, rows, :tiles] = lists_ref[k] if a == 0 else names_ref[a - 1, k]
    for a in range(3):
        counts = tally_ref[...] if a == 0 else sizes_ref[R + a]
        grid_ref[4 + a, :, :tiles] = jnp.broadcast_to(counts, (lines, tiles))
    row = lax.broadcasted_iota(jnp.int32, shape, 0)
    lane = lax.broadcasted_iota(jnp.int32, shape, 1)

    def spread(first):
        second = pltpu.roll(grid_ref[first + 1], tiles, 1)
        return grid_ref[first] + second + pltpu.roll(grid_ref[first + 2], 2 * tiles, 1)

    lower = (wall > 0).astype(jnp.int32)
    upper = (wall < walls - 1).astype(jnp.int32)
    open_lane = jnp.where(
        lane < tiles,
        1,
        jnp.where(lane < 2 * tiles, lower, jnp.where(lane < 3 * tiles, upper, 0)),
    )
    low = jnp.where(lane < tiles, tiles, jnp.where(lane < 2 * tiles, 2 * tiles, 0))
    near = spread(0) - low
    inside = jnp.logical_and(jnp.logical_and(near >= 0, near < tiles), open_lane > 0)
    inside = jnp.logical_and(inside, row < used)
    full = jnp.where(grid_ref[3] > LANES, 1, 0)
    wide = jnp.zeros(shape, jnp.int32)
    for b in range(tiles):
        wide = jnp.where(near == b, jnp.broadcast_to(full[:, b : b + 1], shape), wide)
    groups = lax.shift_right_logical(spread(4) + (ROWS - 1), SHIFT)
    kinds = 2 * top
    kind = jnp.where(inside, top - groups + (1 - wide) * top, -1)
    hits = jnp.concatenate([jnp.where(kind == c, 1.0, 0.0) for c in range(kinds)], axis=0)
    size = kinds * lines
    exact = None if max(3 * tiles, 2 * used * tiles) <= 512 else lax.Precision.HIGHEST

    def dot(left, right):
        if exact is None:
            left, right = left.astype(jnp.bfloat16), right.astype(jnp.bfloat16)
        return jnp.dot(left, right, preferred_element_type=jnp.float32, precision=exact)

    up = lax.broadcasted_iota(jnp.int32, (LANES, LANES), 0)
    across = lax.broadcasted_iota(jnp.int32, (LANES, LANES), 1)
    ahead = dot(hits, jnp.where(up <= across, 1.0, 0.0))
    sums = jnp.broadcast_to(ahead[:, LANES - 1 :], (size, LANES))
    down = lax.broadcasted_iota(jnp.int32, (size, size), 0)
    over = lax.broadcasted_iota(jnp.int32, (size, size), 1)
    home, away = down // lines, over // lines
    same = home == away
    before = dot(jnp.where(jnp.logical_and(same, over < down), 1.0, 0.0), sums)
    total = dot(jnp.where(same, 1.0, 0.0), sums)
    halves_of = lambda value: (jnp.floor(value * 0.5), value - 2.0 * jnp.floor(value * 0.5))
    pairs_of, odd_of = halves_of(total)
    first = jnp.where(jnp.logical_and(away < home, over == away * lines), 1.0, 0.0)
    start = dot(first, pairs_of) * 2.0 + dot(first, odd_of)
    heavy = start[top * lines : top * lines + 1]
    gap = heavy - 2.0 * jnp.floor(heavy * 0.5)
    start = start + jnp.where(down[:, :1] >= top * lines, gap, 0.0)
    spots = start + before + (ahead - hits)
    trash = float(3 * used * tiles + 16)
    place = jnp.full(shape, trash, jnp.float32)
    extra = jnp.full(shape, trash, jnp.float32)
    begin = jnp.zeros(shape, jnp.float32)
    for c in range(kinds):
        part = slice(c * lines, (c + 1) * lines)
        place = jnp.where(hits[part] > 0.0, spots[part], place)
        begin = jnp.where(lane == c, jnp.floor((start[part] + 1.0) * 0.5), begin)
    last = start[size - lines :] + total[size - lines :]
    begin = jnp.where(lane == kinds, jnp.floor((last + 1.0) * 0.5), begin)
    extra = jnp.where(lane == 0, jnp.where(gap > 0.0, heavy, trash), extra)
    for d in range(5):
        extra = jnp.where(lane == 1 + d, last + d, extra)
    at = near + lax.div(row, list_len) * tiles
    code = lax.shift_left(place.astype(jnp.int32), 16) + jnp.where(inside, at, 0)
    code = jnp.where(row == used, extra.astype(jnp.int32), code)
    codes_ref[...] = jnp.where(row == used + 1, begin.astype(jnp.int32), code)


def gather_kernel(
    chans,
    walls,
    coords_in,
    masses_in,
    tally_in,
    lists_in,
    ext_ref,
    over_out,
    codes_out,
    sizes_ref,
    names_ref,
    grid_ref,
    codes_ref,
    coords_ref,
    masses_ref,
    tally_ref,
    lists_ref,
    over_ref,
    own_ref,
    send_sem,
    recv_sem,
    pass_sem,
    size_send,
    size_recv,
    name_send,
    name_recv,
    local_sem,
):
    chan = lax.axis_index("chan")
    wall = lax.axis_index("wall")
    odd = lax.rem(chan, 2)
    twin = chan + 1 - 2 * odd
    sides = (wall > 0).astype(jnp.int32) + (wall < walls - 1).astype(jnp.int32)
    fetches = [
        pltpu.make_async_copy(source, target, local_sem.at[i])
        for i, (source, target) in enumerate(
            (
                (masses_in, masses_ref),
                (tally_in, tally_ref),
                (coords_in, coords_ref),
                (lists_in, lists_ref),
            )
        )
    ]
    for one in fetches:
        one.start()
    sizes_ref[...] = jnp.zeros_like(sizes_ref)
    names_ref[...] = jnp.zeros_like(names_ref)
    barrier = pltpu.get_barrier_semaphore()
    for k in range(1, R + 1):
        target = (lax.rem(chan + k, chans), wall)
        pl.semaphore_signal(barrier, inc=1, device_id=target, device_id_type=MESH)

    @pl.when(odd == 1)
    def _():
        pl.semaphore_signal(barrier, inc=1, device_id=(twin, wall), device_id_type=MESH)

    for _, other, there in wall_cases(wall, walls):
        @pl.when(there)
        def _(other=other):
            pl.semaphore_signal(barrier, inc=1, device_id=(chan, other), device_id_type=MESH)

    tiles, tile_len = over_ref.shape[1:]
    parts = tile_len // LANES
    height = tiles * parts

    def load(ref, base):
        return jnp.concatenate(
            [ref[pl.ds(base + h, tiles, stride=parts), :] for h in range(parts)], axis=1
        )

    spot = lax.broadcasted_iota(jnp.int32, (tiles, tile_len), 0)
    slot = lax.broadcasted_iota(jnp.int32, (tiles, tile_len), 1)
    for one in fetches:
        one.wait()
    tally = jnp.broadcast_to(tally_ref[...].astype(jnp.float32), (tiles, tiles))
    same = spot[:, :tiles] == slot[:, :tiles]
    limit = jnp.sum(jnp.where(same, tally, 0.0), axis=1, keepdims=True)
    filled = slot.astype(jnp.float32) < limit
    mass = load(masses_ref, 0)
    root = jnp.exp(jnp.log(mass) * (1.0 / 3.0))
    root = root - (root * root * root - mass) / (3.0 * root * root)
    over_ref[0] = jnp.where(filled, 1.0, 0.0)
    over_ref[1] = jnp.where(filled, 1.0 / mass, 0.0)
    fields = [load(coords_ref, i * height) for i in range(3)] + [jnp.where(filled, root, 0.0)]
    for i, field in enumerate(fields):
        for h in range(parts):
            own_ref[h, pl.ds(i, tiles, stride=4), :] = field[:, h * LANES : (h + 1) * LANES]

    keep = [
        pltpu.make_async_copy(own_ref, ext_ref.at[0], local_sem.at[0]),
        pltpu.make_async_copy(over_ref, over_out, local_sem.at[1]),
        pltpu.make_async_copy(codes_ref, codes_out, local_sem.at[2]),
    ]
    pl.semaphore_wait(barrier, R + 1 + sides - odd)

    def remote(source, target, sent, got, device):
        return pltpu.make_async_remote_copy(
            src_ref=source,
            dst_ref=target,
            send_sem=sent,
            recv_sem=got,
            device_id=device,
            device_id_type=MESH,
        )

    def behind(k):
        return (lax.rem(chan + chans - k, chans), wall)

    def copy(k):
        return remote(own_ref, ext_ref.at[k], send_sem.at[k], recv_sem.at[k], behind(k))

    def tell(k):
        return remote(tally_ref, sizes_ref.at[k], size_send.at[k], size_recv.at[k], behind(k))

    def aside(side, other, what):
        slab = R + 1 + side
        device = (chan, other)
        source, target, sent, got = (
            (own_ref, ext_ref.at[slab], send_sem.at[slab], recv_sem.at[slab]),
            (tally_ref, sizes_ref.at[slab], size_send.at[slab], size_recv.at[slab]),
            (lists_ref, names_ref.at[side], name_send.at[side], name_recv.at[side]),
        )[what]
        return remote(source, target, sent, got, device)

    def relay(k, own=False):
        into = k - 1 + 2 * odd
        source = own_ref if own else ext_ref.at[k]
        return remote(source, ext_ref.at[into], pass_sem.at[into], recv_sem.at[into], (twin, wall))

    for k in range(1, R + 1):
        tell(k).start()
    for side, other, there in wall_cases(wall, walls):
        @pl.when(there)
        def _(side=side, other=other):
            for what in (1, 2):
                aside(1 - side, other, what).start()

    copy(2).start()
    copy(4).start()
    for side, other, there in wall_cases(wall, walls):
        @pl.when(there)
        def _(side=side, other=other):
            aside(1 - side, other, 0).start()

    @pl.when(odd == 1)
    def _():
        relay(0, True).start()

    for one in keep[:2]:
        one.start()
    for k in range(1, R + 1):
        tell(k).wait()
    for side, other, there in wall_cases(wall, walls):
        @pl.when(there)
        def _(side=side, other=other):
            for what in (1, 2):
                aside(side, other, what).wait_recv()
                aside(1 - side, other, what).wait_send()

    arrange(wall, walls, tiles, tile_len, lists_ref, names_ref, tally_ref, sizes_ref, grid_ref, codes_ref)
    keep[2].start()

    @pl.when(odd == 0)
    def _():
        for k in (2, 4):
            copy(k).wait_recv()
            relay(k).start()

    @pl.when(odd == 1)
    def _():
        copy(2).wait_recv()
        relay(2).start()
        copy(4).wait_recv()

    for side, other, there in wall_cases(wall, walls):
        @pl.when(there)
        def _(side=side, other=other):
            aside(side, other, 0).wait_recv()
            aside(1 - side, other, 0).wait_send()

    copy(1).wait_recv()
    copy(3).wait_recv()
    copy(2).wait_send()
    copy(4).wait_send()

    @pl.when(odd == 0)
    def _():
        relay(2).wait_send()
        relay(4).wait_send()

    @pl.when(odd == 1)
    def _():
        relay(0, True).wait_send()
        relay(2).wait_send()

    for one in keep:
        one.wait()


def gather(coords, masses, counts, lists, chans, walls):
    slabs = R + 3
    tiles = counts.shape[0]
    tile_len = masses.shape[0] * LANES // tiles
    hbm = pl.BlockSpec(memory_space=pl.ANY)
    block = (tile_len // LANES, 4 * tiles, LANES)
    tally = counts.reshape(1, tiles)
    lines = -(-((R + 1) * lists.shape[1] + 2) // 8) * 8
    many = pltpu.SemaphoreType.DMA((slabs,))
    few = pltpu.SemaphoreType.DMA((2,))
    return pl.pallas_call(
        functools.partial(gather_kernel, chans, walls),
        out_shape=(
            jax.ShapeDtypeStruct((slabs,) + block, jnp.float32),
            jax.ShapeDtypeStruct((2, tiles, tile_len), jnp.float32),
            jax.ShapeDtypeStruct((lines, LANES), jnp.int32),
        ),
        in_specs=[hbm] * 4,
        out_specs=(hbm,) * 3,
        scratch_shapes=[
            pltpu.VMEM((slabs,) + tally.shape, jnp.int32),
            pltpu.VMEM((2,) + lists.shape, jnp.int32),
            pltpu.VMEM((7, lines, LANES), jnp.int32),
            pltpu.VMEM((lines, LANES), jnp.int32),
            pltpu.VMEM(coords.shape, jnp.float32),
            pltpu.VMEM(masses.shape, jnp.float32),
            pltpu.VMEM(tally.shape, jnp.int32),
            pltpu.VMEM(lists.shape, jnp.int32),
            pltpu.VMEM((2, tiles, tile_len), jnp.float32),
            pltpu.VMEM(block, jnp.float32),
            many,
            many,
            many,
            many,
            many,
            few,
            few,
            pltpu.SemaphoreType.DMA((4,)),
        ],
        compiler_params=pltpu.CompilerParams(collective_id=0, has_side_effects=True),
    )(coords, masses, tally, lists)


def splits(v):
    first = v.astype(jnp.bfloat16).astype(jnp.float32)
    rest = v - first
    second = rest.astype(jnp.bfloat16).astype(jnp.float32)
    third = (rest - second).astype(jnp.bfloat16).astype(jnp.float32)
    return first, second, third


def halves(block, row):
    low = jnp.broadcast_to(block[row : row + 1], block.shape)
    high = jnp.broadcast_to(block[row + 4 : row + 5], block.shape)
    spot = lax.broadcasted_iota(jnp.int32, block.shape, 0)
    return low, high, jnp.where(spot < 4, low, high)


def pair_kernel(
    walls,
    codes_in,
    far_ref,
    gained_ref,
    handed_ref,
    afeat,
    wcol,
    bfeat,
    brow,
    gacc,
    hands,
    codes,
    items,
    ext_ref,
    load_sem,
    code_sem,
):
    _, tiles, tile_len = gained_ref.shape
    slots = (R + 1) * tiles
    parts = tile_len // LANES
    wall = lax.axis_index("wall")
    near = ((0, wall > 0), (1, wall < walls - 1))
    slabs = far_ref.shape[0]

    def bring(at):
        return pltpu.make_async_copy(far_ref.at[at], ext_ref.at[at], load_sem.at[at])

    decode = pltpu.make_async_copy(codes_in, codes, code_sem)
    bring(0).start()
    decode.start()
    for side, there in near:
        pl.when(there)(lambda side=side: bring(R + 1 + side).start())
    for k in range(1, R + 1):
        bring(k).start()
    classes = 2 * (tile_len // ROWS)
    used = (R + 1) * NB

    def block_of(slab, i):
        rows = pl.ds(pl.multiple_of(i * 8, 8), 8)
        return jnp.concatenate([ext_ref[slab, h, rows, :] for h in range(parts)], axis=1)

    spot = lax.broadcasted_iota(jnp.int32, (8, tile_len), 0)
    part = jnp.bitwise_and(spot, 3)
    quarter = 1.0 / R
    base = jnp.where(part == 0, -0.5, jnp.where(part == 3, 0.0, -float(R))) * quarter
    scale = jnp.where(part == 3, 1.0, quarter)

    def own_pair(i, a):
        block = block_of((0, R + 1, R + 2)[a], i)
        _, _, s = halves(block, 3)
        lift = jnp.where(part == 1, (0.0, -2.0, 2.0)[a], 0.0)
        place = jnp.where(part == 3, 0.0, block * scale + (base + lift))
        square = place * place
        pairsum = square + pltpu.roll(square, 1, 0)
        total = pairsum + pltpu.roll(pairsum, 2, 0)
        full = jnp.where(part == 3, total, place)
        one, two, three = splits(full)
        ones = jnp.where(part == 3, 1.0, 0.0)
        weight = s * s * s
        rest = jnp.zeros((LANES - 80, tile_len), jnp.float32)
        stack = jnp.concatenate(
            [one, one, two, two, one, three, ones, ones, ones, weight, rest], axis=0
        )
        turned = jnp.transpose(stack, (1, 0))
        lane = lax.broadcasted_iota(jnp.int32, turned.shape, 1)
        low = jnp.bitwise_and(lane, 4) == 0
        inside = lane < 72
        for half in range(2):
            t = 2 * i + half + a * tiles
            keep = low if half == 0 else jnp.logical_not(low)
            mine = jnp.where(jnp.logical_and(keep, inside), turned, 0.0)
            other = pltpu.roll(mine, 4 if half == 0 else LANES - 4, 1)
            afeat[half * 3 * tiles + t] = mine.astype(jnp.bfloat16)
            afeat[(1 - half) * 3 * tiles + t] = other.astype(jnp.bfloat16)
            wcol[t] = jnp.broadcast_to(
                turned[:, 72 + 4 * half : 73 + 4 * half], (tile_len, LANES)
            )

    def enlist(t, a):
        spot = t + a * tiles
        high_bits = lax.shift_left(spot, 16)
        for r in range(used):
            code = codes[r, spot]
            items[lax.shift_right_logical(code, 16)] = high_bits + jnp.bitwise_and(code, 65535)

    def prepare(a):
        bring((0, R + 1, R + 2)[a]).wait()

        def pair_of(i, carry):
            enlist(2 * i, a)
            enlist(2 * i + 1, a)
            own_pair(i, a)
            return carry

        lax.fori_loop(0, tiles // 2, pair_of, 0)

    hands[...] = jnp.zeros_like(hands)

    def clear(t, carry):
        gacc[t] = jnp.zeros((tile_len, LANES), jnp.float32)
        return carry

    lax.fori_loop(0, 3 * tiles, clear, 0)
    decode.wait()
    prepare(0)
    for side, there in near:
        pl.when(there)(functools.partial(prepare, side + 1))
    for k in range(1, R + 1):
        bring(k).wait()

    def ext_pair(i, k):
        at = k * (tiles // 2) + i
        block = block_of(k, i)
        low, high, s = halves(block, 3)
        filled = s > 0.0
        place = block * scale + (base + jnp.where(part == 0, k * quarter, 0.0))
        place = jnp.where(jnp.logical_and(part < 3, filled), place, 0.0)
        s = jnp.where(filled, s, 1.0)
        s2 = s * s
        square = place * place
        pairsum = square + pltpu.roll(square, 1, 0)
        total = pairsum + pltpu.roll(pairsum, 2, 0)
        tail = jnp.where(filled, s2 * (total + 0.0001 / (R * R)), 128.0)
        full = jnp.where(part == 3, s2, -2.0 * s2 * place)
        one, two, three = splits(full)
        first, second, third = splits(tail)
        stack = jnp.concatenate(
            [one, two, one, two, three, one, first, second, third, jnp.zeros_like(one)],
            axis=0,
        )
        bfeat[at] = stack.astype(jnp.bfloat16)
        for half, root in enumerate((low, high)):
            root = jnp.where(root > 0.0, root, 1.0)
            brow[at * 2 + half, :8] = 2.0 * root
            brow[at * 2 + half, 8:] = 4.0 * root * root * root

    def ext_pairs(i, carry):
        for k in range(R + 1):
            ext_pair(i, k)
        return carry

    lax.fori_loop(0, tiles // 2, ext_pairs, 0)
    nothing = ((3 * tiles) << 16) + slots
    for c in range(6):
        items[codes[used, c]] = nothing
    ends = [codes[used + 1, c] for c in range(classes + 1)]

    def body(*accs):
        pieces = tile_len // PIECE
        for ref in accs:
            pltpu.matmul_pop(ref)

        def fields(m):
            packed = items[m]
            at = jnp.bitwise_and(packed, 65535)
            return at, lax.shift_right_logical(packed, 16)

        def push(m, q):
            at, _ = fields(m)
            rhs = jnp.concatenate(
                [
                    bfeat[lax.shift_right_logical(at, 1)],
                    jnp.zeros((256 - 80, tile_len), jnp.bfloat16),
                ],
                axis=0,
            )
            pltpu.matmul_push_rhs(rhs, staging_register=0, mxu_index=q)

        def feed(which, q, p):
            lhs = afeat[which, p * PIECE : (p + 1) * PIECE]
            lhs = jnp.concatenate([lhs, jnp.zeros((PIECE, 256 - LANES), jnp.bfloat16)], axis=1)
            pltpu.matmul_acc_lhs(
                accs[q * pieces + p], lhs, load_staged_rhs=0 if p == 0 else None
            )

        def which_of(m):
            at, t = fields(m)
            return jnp.bitwise_and(at, 1) * (3 * tiles) + t

        def run(j, carry, groups, width):
            now = [fields(2 * j + q) for q in range(2)]
            then = [which_of(2 * j + 2 + q) for q in range(2)]
            rows = [
                [brow[at, r * 8 : r * 8 + 8, h * LANES : (h + 1) * LANES] for r in range(2) for h in range(width)]
                for at, _ in now
            ]
            sums = [[None] * width for _ in now]
            for p in range(pieces if width > 1 else groups * ROWS // PIECE):
                for q, (at, t) in enumerate(now):
                    u = pltpu.matmul_pop(accs[q * pieces + p])
                    feed(then[q], q, p)
                    if p == 0:
                        push(2 * j + 4 + q, q)
                    if p >= groups * ROWS // PIECE:
                        continue
                    for r in range(0, PIECE, 8):
                        here = pl.ds(p * PIECE + r, 8)
                        aw = wcol[t, here, :]
                        total = None
                        for h in range(width):
                            v = u[r : r + 8, h * LANES : (h + 1) * LANES]
                            o = jnp.maximum(rows[q][h] - v * lax.rsqrt(v), 0.0)
                            w = jnp.minimum(o * o * o, rows[q][width + h] - (v * o) * 3.0)
                            total = w if total is None else total + w
                            back = w * aw
                            sums[q][h] = back if sums[q][h] is None else sums[q][h] + back
                        gacc[t, here, :] += total
            for q, (at, t) in enumerate(now):
                for h in range(width):
                    hands[at, :, h * LANES : (h + 1) * LANES] += sums[q][h]
            return carry

        for q in range(2):
            push(q, q)
        for q in range(2):
            for p in range(pieces):
                feed(which_of(q), q, p)
        for q in range(2):
            push(2 + q, q)
        for c in range(classes):
            top = classes // 2
            lax.fori_loop(
                ends[c],
                ends[c + 1],
                functools.partial(run, groups=top - c % top, width=2 - c // top),
                0,
            )
        for q in range(2):
            for p in range(pieces):
                feed(which_of(q), q, p)
        for ref in accs:
            pltpu.matmul_pop(ref)

    pl.run_scoped(
        body,
        *[pltpu.ACC(q)((PIECE, 256), jnp.float32) for q in range(2) for _ in range(tile_len // PIECE)],
    )
    lane = lax.broadcasted_iota(jnp.int32, (tile_len, LANES), 1)

    def finish(a):
        columns = jnp.zeros((tile_len, LANES), jnp.float32)
        for t in range(tiles):
            value = jnp.sum(gacc[a * tiles + t], axis=1, keepdims=True)
            columns = jnp.where(lane == t, value, columns)
        gained_ref[a] = jnp.transpose(columns, (1, 0))[:tiles]

    finish(0)
    for side, there in near:
        pl.when(there)(functools.partial(finish, side + 1))
    handed_ref[...] = jnp.sum(hands[tiles:slots], axis=1).reshape(handed_ref.shape)


def pairs(codes, ext, walls):
    tiles = ext.shape[2] // 4
    tile_len = ext.shape[1] * LANES
    hbm = pl.BlockSpec(memory_space=pl.ANY)
    vmem = pl.BlockSpec(memory_space=pltpu.VMEM)
    slots = (R + 1) * tiles
    entries = 3 * slots * NB
    return pl.pallas_call(
        functools.partial(pair_kernel, walls),
        out_shape=(
            jax.ShapeDtypeStruct((3, tiles, tile_len), jnp.float32),
            jax.ShapeDtypeStruct((R, tiles, tile_len), jnp.float32),
        ),
        in_specs=[hbm, hbm],
        out_specs=(vmem, vmem),
        scratch_shapes=[
            pltpu.VMEM((6 * tiles, tile_len, LANES), jnp.bfloat16),
            pltpu.VMEM((3 * tiles + 1, tile_len, LANES), jnp.float32),
            pltpu.VMEM((slots // 2 + 1, 80, tile_len), jnp.bfloat16),
            pltpu.VMEM((slots + 1, 16, tile_len), jnp.float32),
            pltpu.VMEM((3 * tiles + 1, tile_len, LANES), jnp.float32),
            pltpu.VMEM((slots + 1, 8, tile_len), jnp.float32),
            pltpu.SMEM(codes.shape, jnp.int32),
            pltpu.SMEM((entries + 32,), jnp.int32),
            pltpu.VMEM(ext.shape, jnp.float32),
            pltpu.SemaphoreType.DMA((ext.shape[0],)),
            pltpu.SemaphoreType.DMA,
        ],
    )(codes, ext)


def return_kernel(
    chans,
    walls,
    gained_in,
    handed_in,
    over_in,
    out_ref,
    gained_ref,
    handed_ref,
    over_ref,
    held,
    hold,
    send_sem,
    recv_sem,
    local_sem,
):
    chan = lax.axis_index("chan")
    wall = lax.axis_index("wall")
    sides = (wall > 0).astype(jnp.int32) + (wall < walls - 1).astype(jnp.int32)
    pulls = [
        pltpu.make_async_copy(source, target, local_sem.at[i])
        for i, (source, target) in enumerate(
            ((handed_in, handed_ref), (gained_in, gained_ref), (over_in, over_ref))
        )
    ]
    for one in pulls:
        one.start()
    barrier = pltpu.get_barrier_semaphore()
    for k in range(1, R + 1):
        target = (lax.rem(chan + chans - k, chans), wall)
        pl.semaphore_signal(barrier, inc=1, device_id=target, device_id_type=MESH)
    for _, other, there in wall_cases(wall, walls):
        @pl.when(there)
        def _(other=other):
            pl.semaphore_signal(barrier, inc=1, device_id=(chan, other), device_id_type=MESH)
    for one in pulls:
        one.wait()
    pl.semaphore_wait(barrier, R + sides)

    def copy(source, slot, device):
        return pltpu.make_async_remote_copy(
            src_ref=source,
            dst_ref=held.at[slot],
            send_sem=send_sem.at[slot],
            recv_sem=recv_sem.at[slot],
            device_id=device,
            device_id_type=MESH,
        )

    def ahead(k):
        return copy(handed_ref.at[k - 1], k - 1, (lax.rem(chan + k, chans), wall))

    def aside(side, slot, other):
        return copy(gained_ref.at[side + 1], R + slot, (chan, other))

    for k in range(R, 0, -1):
        ahead(k).start()
    for side, other, there in wall_cases(wall, walls):
        @pl.when(there)
        def _(side=side, other=other):
            aside(side, 1 - side, other).start()

    tiles = hold.shape[0]
    hold[...] = gained_ref[0]
    for side, other, there in wall_cases(wall, walls):
        @pl.when(there)
        def _(side=side, other=other):
            aside(side, side, other).wait_recv()
            hold[...] += held[R + side]

    handed = None
    for k in range(1, R + 1):
        ahead(k).wait_recv()
        handed = held[k - 1] if handed is None else handed + held[k - 1]
    total = hold[...] * over_ref[0] + handed * over_ref[1]
    parts = hold.shape[1] // LANES
    for h in range(parts):
        out_ref[pl.ds(h, tiles, stride=parts), :] = total[:, h * LANES : (h + 1) * LANES]
    for k in range(1, R + 1):
        ahead(k).wait_send()
    for side, other, there in wall_cases(wall, walls):
        @pl.when(there)
        def _(side=side, other=other):
            aside(side, 1 - side, other).wait_send()


def hand_back(gained, handed, over, chans, walls):
    _, tiles, tile_len = gained.shape
    vmem = pl.BlockSpec(memory_space=pltpu.VMEM)
    return pl.pallas_call(
        functools.partial(return_kernel, chans, walls),
        out_shape=jax.ShapeDtypeStruct((tiles * tile_len // LANES, LANES), gained.dtype),
        in_specs=[pl.BlockSpec(memory_space=pl.ANY)] * 3,
        out_specs=vmem,
        scratch_shapes=[
            pltpu.VMEM(gained.shape, jnp.float32),
            pltpu.VMEM(handed.shape, jnp.float32),
            pltpu.VMEM(over.shape, jnp.float32),
            pltpu.VMEM((R + 2, tiles, tile_len), jnp.float32),
            pltpu.VMEM((tiles, tile_len), jnp.float32),
            pltpu.SemaphoreType.DMA((R + 2,)),
            pltpu.SemaphoreType.DMA((R + 2,)),
            pltpu.SemaphoreType.DMA((3,)),
        ],
        compiler_params=pltpu.CompilerParams(collective_id=1, has_side_effects=True),
    )(gained, handed, over)


def on_device(chans, walls, coords, masses, counts, lists):
    tiles = counts.shape[2]
    tile_len = masses.shape[2] // tiles
    scale = 1.0 / (4.0 * math.pi * NB * tile_len)
    lists = jnp.swapaxes(lists.reshape(lists.shape[2:]), 1, 2)
    ext, over, codes = gather(
        coords.reshape(-1, LANES),
        masses.reshape(-1, LANES),
        counts.reshape(-1),
        lists,
        chans,
        walls,
    )
    gained, handed = pairs(codes, ext, walls)
    total = hand_back(gained, handed, over, chans, walls)
    return total.reshape(1, 1, -1) * scale


def solution(mesh):
    placed = (
        P(None, "chan", "wall", None),
        P("chan", "wall", None),
        P("chan", "wall", None),
        P("chan", "wall", None, None, None),
    )
    body = functools.partial(on_device, mesh.shape["chan"], mesh.shape["wall"])
    return jax.shard_map(
        body, mesh=mesh, in_specs=placed, out_specs=P("chan", "wall", None), check_vma=False
    )
```

```python
import functools
import math

import jax
import jax.numpy as jnp
from jax import lax
from jax.experimental import pallas as pl
from jax.experimental.pallas import tpu as pltpu
from jax.sharding import PartitionSpec as P

NB = 2
R = 4
LANES = 128
ROWS = 32
SHIFT = 5
PIECE = 32
MESH = pl.DeviceIdType.MESH


def wall_cases(wall, walls):
    return [(0, wall - 1, wall > 0), (1, wall + 1, wall < walls - 1)]


def arrange(
    wall, walls, tiles, tile_len, lists_ref, names_ref, tally_ref, sizes_ref, grid_ref, codes_ref
):
    list_len = lists_ref.shape[1]
    lines = codes_ref.shape[0]
    used = (R + 1) * list_len
    top = tile_len // ROWS
    shape = (lines, LANES)
    grid_ref[...] = jnp.zeros_like(grid_ref)
    for k in range(R + 1):
        rows = pl.ds(k * list_len, list_len)
        counts = tally_ref[...] if k == 0 else sizes_ref[k]
        grid_ref[3, rows, :tiles] = jnp.broadcast_to(counts, (list_len, tiles))
        for a in range(3):
            grid_ref[a, rows, :tiles] = lists_ref[k] if a == 0 else names_ref[a - 1, k]
    for a in range(3):
        counts = tally_ref[...] if a == 0 else sizes_ref[R + a]
        grid_ref[4 + a, :, :tiles] = jnp.broadcast_to(counts, (lines, tiles))
    row = lax.broadcasted_iota(jnp.int32, shape, 0)
    lane = lax.broadcasted_iota(jnp.int32, shape, 1)

    def spread(first):
        second = pltpu.roll(grid_ref[first + 1], tiles, 1)
        return grid_ref[first] + second + pltpu.roll(grid_ref[first + 2], 2 * tiles, 1)

    lower = (wall > 0).astype(jnp.int32)
    upper = (wall < walls - 1).astype(jnp.int32)
    open_lane = jnp.where(
        lane < tiles,
        1,
        jnp.where(lane < 2 * tiles, lower, jnp.where(lane < 3 * tiles, upper, 0)),
    )
    low = jnp.where(lane < tiles, tiles, jnp.where(lane < 2 * tiles, 2 * tiles, 0))
    near = spread(0) - low
    inside = jnp.logical_and(jnp.logical_and(near >= 0, near < tiles), open_lane > 0)
    inside = jnp.logical_and(inside, row < used)
    full = jnp.where(grid_ref[3] > LANES, 1, 0)
    wide = jnp.zeros(shape, jnp.int32)
    for b in range(tiles):
        wide = jnp.where(near == b, jnp.broadcast_to(full[:, b : b + 1], shape), wide)
    groups = lax.shift_right_logical(spread(4) + (ROWS - 1), SHIFT)
    kinds = 2 * top
    kind = jnp.where(inside, top - groups + (1 - wide) * top, -1)
    hits = jnp.concatenate([jnp.where(kind == c, 1.0, 0.0) for c in range(kinds)], axis=0)
    size = kinds * lines
    exact = None if max(3 * tiles, 2 * used * tiles) <= 512 else lax.Precision.HIGHEST

    def dot(left, right):
        if exact is None:
            left, right = left.astype(jnp.bfloat16), right.astype(jnp.bfloat16)
        return jnp.dot(left, right, preferred_element_type=jnp.float32, precision=exact)

    up = lax.broadcasted_iota(jnp.int32, (LANES, LANES), 0)
    across = lax.broadcasted_iota(jnp.int32, (LANES, LANES), 1)
    ahead = dot(hits, jnp.where(up <= across, 1.0, 0.0))
    sums = jnp.broadcast_to(ahead[:, LANES - 1 :], (size, LANES))
    down = lax.broadcasted_iota(jnp.int32, (size, size), 0)
    over = lax.broadcasted_iota(jnp.int32, (size, size), 1)
    home, away = down // lines, over // lines
    same = home == away
    before = dot(jnp.where(jnp.logical_and(same, over < down), 1.0, 0.0), sums)
    total = dot(jnp.where(same, 1.0, 0.0), sums)
    halves_of = lambda value: (jnp.floor(value * 0.5), value - 2.0 * jnp.floor(value * 0.5))
    pairs_of, odd_of = halves_of(total)
    first = jnp.where(jnp.logical_and(away < home, over == away * lines), 1.0, 0.0)
    start = dot(first, pairs_of) * 2.0 + dot(first, odd_of)
    heavy = start[top * lines : top * lines + 1]
    gap = heavy - 2.0 * jnp.floor(heavy * 0.5)
    start = start + jnp.where(down[:, :1] >= top * lines, gap, 0.0)
    spots = start + before + (ahead - hits)
    trash = float(3 * used * tiles + 16)
    place = jnp.full(shape, trash, jnp.float32)
    extra = jnp.full(shape, trash, jnp.float32)
    begin = jnp.zeros(shape, jnp.float32)
    for c in range(kinds):
        part = slice(c * lines, (c + 1) * lines)
        place = jnp.where(hits[part] > 0.0, spots[part], place)
        begin = jnp.where(lane == c, jnp.floor((start[part] + 1.0) * 0.5), begin)
    last = start[size - lines :] + total[size - lines :]
    begin = jnp.where(lane == kinds, jnp.floor((last + 1.0) * 0.5), begin)
    extra = jnp.where(lane == 0, jnp.where(gap > 0.0, heavy, trash), extra)
    for d in range(5):
        extra = jnp.where(lane == 1 + d, last + d, extra)
    at = near + lax.div(row, list_len) * tiles
    code = lax.shift_left(place.astype(jnp.int32), 16) + jnp.where(inside, at, 0)
    code = jnp.where(row == used, extra.astype(jnp.int32), code)
    codes_ref[...] = jnp.where(row == used + 1, begin.astype(jnp.int32), code)


def gather_kernel(
    chans,
    walls,
    coords_in,
    masses_in,
    tally_in,
    lists_in,
    ext_ref,
    over_out,
    codes_out,
    sizes_ref,
    names_ref,
    grid_ref,
    codes_ref,
    coords_ref,
    masses_ref,
    tally_ref,
    lists_ref,
    over_ref,
    own_ref,
    send_sem,
    recv_sem,
    pass_sem,
    size_send,
    size_recv,
    name_send,
    name_recv,
    local_sem,
):
    chan = lax.axis_index("chan")
    wall = lax.axis_index("wall")
    odd = lax.rem(chan, 2)
    twin = chan + 1 - 2 * odd
    sides = (wall > 0).astype(jnp.int32) + (wall < walls - 1).astype(jnp.int32)
    fetches = [
        pltpu.make_async_copy(source, target, local_sem.at[i])
        for i, (source, target) in enumerate(
            (
                (masses_in, masses_ref),
                (tally_in, tally_ref),
                (coords_in, coords_ref),
                (lists_in, lists_ref),
            )
        )
    ]
    for one in fetches:
        one.start()
    sizes_ref[...] = jnp.zeros_like(sizes_ref)
    names_ref[...] = jnp.zeros_like(names_ref)
    barrier = pltpu.get_barrier_semaphore()
    for k in range(1, R + 1):
        target = (lax.rem(chan + k, chans), wall)
        pl.semaphore_signal(barrier, inc=1, device_id=target, device_id_type=MESH)

    @pl.when(odd == 1)
    def _():
        pl.semaphore_signal(barrier, inc=1, device_id=(twin, wall), device_id_type=MESH)

    for _, other, there in wall_cases(wall, walls):
        @pl.when(there)
        def _(other=other):
            pl.semaphore_signal(barrier, inc=1, device_id=(chan, other), device_id_type=MESH)

    tiles, tile_len = over_ref.shape[1:]
    parts = tile_len // LANES
    height = tiles * parts

    def load(ref, base):
        return jnp.concatenate(
            [ref[pl.ds(base + h, tiles, stride=parts), :] for h in range(parts)], axis=1
        )

    spot = lax.broadcasted_iota(jnp.int32, (tiles, tile_len), 0)
    slot = lax.broadcasted_iota(jnp.int32, (tiles, tile_len), 1)
    for one in fetches:
        one.wait()
    tally = jnp.broadcast_to(tally_ref[...].astype(jnp.float32), (tiles, tiles))
    same = spot[:, :tiles] == slot[:, :tiles]
    limit = jnp.sum(jnp.where(same, tally, 0.0), axis=1, keepdims=True)
    filled = slot.astype(jnp.float32) < limit
    mass = load(masses_ref, 0)
    root = jnp.exp(jnp.log(mass) * (1.0 / 3.0))
    root = root - (root * root * root - mass) / (3.0 * root * root)
    over_ref[0] = jnp.where(filled, 1.0, 0.0)
    over_ref[1] = jnp.where(filled, 1.0 / mass, 0.0)
    fields = [load(coords_ref, i * height) for i in range(3)] + [jnp.where(filled, root, 0.0)]
    for i, field in enumerate(fields):
        for h in range(parts):
            own_ref[h, pl.ds(i, tiles, stride=4), :] = field[:, h * LANES : (h + 1) * LANES]

    keep = [
        pltpu.make_async_copy(own_ref, ext_ref.at[0], local_sem.at[0]),
        pltpu.make_async_copy(over_ref, over_out, local_sem.at[1]),
        pltpu.make_async_copy(codes_ref, codes_out, local_sem.at[2]),
    ]
    pl.semaphore_wait(barrier, R + 1 + sides - odd)

    def remote(source, target, sent, got, device):
        return pltpu.make_async_remote_copy(
            src_ref=source,
            dst_ref=target,
            send_sem=sent,
            recv_sem=got,
            device_id=device,
            device_id_type=MESH,
        )

    def behind(k):
        return (lax.rem(chan + chans - k, chans), wall)

    def copy(k):
        return remote(own_ref, ext_ref.at[k], send_sem.at[k], recv_sem.at[k], behind(k))

    def tell(k):
        return remote(tally_ref, sizes_ref.at[k], size_send.at[k], size_recv.at[k], behind(k))

    def aside(side, other, what):
        slab = R + 1 + side
        device = (chan, other)
        source, target, sent, got = (
            (own_ref, ext_ref.at[slab], send_sem.at[slab], recv_sem.at[slab]),
            (tally_ref, sizes_ref.at[slab], size_send.at[slab], size_recv.at[slab]),
            (lists_ref, names_ref.at[side], name_send.at[side], name_recv.at[side]),
        )[what]
        return remote(source, target, sent, got, device)

    def relay(k, own=False):
        into = k - 1 + 2 * odd
        source = own_ref if own else ext_ref.at[k]
        return remote(source, ext_ref.at[into], pass_sem.at[into], recv_sem.at[into], (twin, wall))

    for k in range(1, R + 1):
        tell(k).start()
    for side, other, there in wall_cases(wall, walls):
        @pl.when(there)
        def _(side=side, other=other):
            for what in (1, 2):
                aside(1 - side, other, what).start()

    copy(2).start()
    copy(4).start()
    for side, other, there in wall_cases(wall, walls):
        @pl.when(there)
        def _(side=side, other=other):
            aside(1 - side, other, 0).start()

    @pl.when(odd == 1)
    def _():
        relay(0, True).start()

    for one in keep[:2]:
        one.start()
    for k in range(1, R + 1):
        tell(k).wait()
    for side, other, there in wall_cases(wall, walls):
        @pl.when(there)
        def _(side=side, other=other):
            for what in (1, 2):
                aside(side, other, what).wait_recv()
                aside(1 - side, other, what).wait_send()

    arrange(wall, walls, tiles, tile_len, lists_ref, names_ref, tally_ref, sizes_ref, grid_ref, codes_ref)
    keep[2].start()

    @pl.when(odd == 0)
    def _():
        for k in (2, 4):
            copy(k).wait_recv()
            relay(k).start()

    @pl.when(odd == 1)
    def _():
        copy(2).wait_recv()
        relay(2).start()
        copy(4).wait_recv()

    for side, other, there in wall_cases(wall, walls):
        @pl.when(there)
        def _(side=side, other=other):
            aside(side, other, 0).wait_recv()
            aside(1 - side, other, 0).wait_send()

    copy(1).wait_recv()
    copy(3).wait_recv()
    copy(2).wait_send()
    copy(4).wait_send()

    @pl.when(odd == 0)
    def _():
        relay(2).wait_send()
        relay(4).wait_send()

    @pl.when(odd == 1)
    def _():
        relay(0, True).wait_send()
        relay(2).wait_send()

    for one in keep:
        one.wait()


def gather(coords, masses, counts, lists, chans, walls):
    slabs = R + 3
    tiles = counts.shape[0]
    tile_len = masses.shape[0] * LANES // tiles
    hbm = pl.BlockSpec(memory_space=pl.ANY)
    block = (tile_len // LANES, 4 * tiles, LANES)
    tally = counts.reshape(1, tiles)
    lines = -(-((R + 1) * lists.shape[1] + 2) // 8) * 8
    many = pltpu.SemaphoreType.DMA((slabs,))
    few = pltpu.SemaphoreType.DMA((2,))
    return pl.pallas_call(
        functools.partial(gather_kernel, chans, walls),
        out_shape=(
            jax.ShapeDtypeStruct((slabs,) + block, jnp.float32),
            jax.ShapeDtypeStruct((2, tiles, tile_len), jnp.float32),
            jax.ShapeDtypeStruct((lines, LANES), jnp.int32),
        ),
        in_specs=[hbm] * 4,
        out_specs=(hbm,) * 3,
        scratch_shapes=[
            pltpu.VMEM((slabs,) + tally.shape, jnp.int32),
            pltpu.VMEM((2,) + lists.shape, jnp.int32),
            pltpu.VMEM((7, lines, LANES), jnp.int32),
            pltpu.VMEM((lines, LANES), jnp.int32),
            pltpu.VMEM(coords.shape, jnp.float32),
            pltpu.VMEM(masses.shape, jnp.float32),
            pltpu.VMEM(tally.shape, jnp.int32),
            pltpu.VMEM(lists.shape, jnp.int32),
            pltpu.VMEM((2, tiles, tile_len), jnp.float32),
            pltpu.VMEM(block, jnp.float32),
            many,
            many,
            many,
            many,
            many,
            few,
            few,
            pltpu.SemaphoreType.DMA((4,)),
        ],
        compiler_params=pltpu.CompilerParams(collective_id=0, has_side_effects=True),
    )(coords, masses, tally, lists)


def splits(v):
    first = v.astype(jnp.bfloat16).astype(jnp.float32)
    rest = v - first
    second = rest.astype(jnp.bfloat16).astype(jnp.float32)
    third = (rest - second).astype(jnp.bfloat16).astype(jnp.float32)
    return first, second, third


def halves(block, row):
    low = jnp.broadcast_to(block[row : row + 1], block.shape)
    high = jnp.broadcast_to(block[row + 4 : row + 5], block.shape)
    spot = lax.broadcasted_iota(jnp.int32, block.shape, 0)
    return low, high, jnp.where(spot < 4, low, high)


def pair_kernel(
    walls,
    codes_in,
    far_ref,
    gained_ref,
    handed_ref,
    afeat,
    wcol,
    bfeat,
    brow,
    gacc,
    hands,
    codes,
    items,
    ext_ref,
    load_sem,
    code_sem,
):
    _, tiles, tile_len = gained_ref.shape
    slots = (R + 1) * tiles
    parts = tile_len // LANES
    wall = lax.axis_index("wall")
    near = ((0, wall > 0), (1, wall < walls - 1))
    slabs = far_ref.shape[0]

    def bring(at):
        return pltpu.make_async_copy(far_ref.at[at], ext_ref.at[at], load_sem.at[at])

    decode = pltpu.make_async_copy(codes_in, codes, code_sem)
    bring(0).start()
    decode.start()
    for side, there in near:
        pl.when(there)(lambda side=side: bring(R + 1 + side).start())
    for k in range(1, R + 1):
        bring(k).start()
    classes = 2 * (tile_len // ROWS)
    used = (R + 1) * NB

    def block_of(slab, i):
        rows = pl.ds(pl.multiple_of(i * 8, 8), 8)
        return jnp.concatenate([ext_ref[slab, h, rows, :] for h in range(parts)], axis=1)

    spot = lax.broadcasted_iota(jnp.int32, (8, tile_len), 0)
    part = jnp.bitwise_and(spot, 3)
    quarter = 1.0 / R
    base = jnp.where(part == 0, -0.5, jnp.where(part == 3, 0.0, -float(R))) * quarter
    scale = jnp.where(part == 3, 1.0, quarter)

    def own_pair(i, a, accs, past):
        block = block_of((0, R + 1, R + 2)[a], i)
        _, _, s = halves(block, 3)
        lift = jnp.where(part == 1, (0.0, -2.0, 2.0)[a], 0.0)
        place = jnp.where(part == 3, 0.0, block * scale + (base + lift))
        square = place * place
        pairsum = square + pltpu.roll(square, 1, 0)
        total = pairsum + pltpu.roll(pairsum, 2, 0)
        full = jnp.where(part == 3, total, place)
        one, two, three = splits(full)
        ones = jnp.where(part == 3, 1.0, 0.0)
        weight = splits(s * s * s)
        rest = jnp.zeros((LANES - 96, tile_len), jnp.float32)
        stack = jnp.concatenate(
            [one, one, two, two, one, three, ones, ones, ones, *weight, rest], axis=0
        )
        turned = jnp.transpose(stack, (1, 0))
        lane = lax.broadcasted_iota(jnp.int32, turned.shape, 1)
        low = jnp.bitwise_and(lane, 4) == 0
        for half in range(2):
            t = 2 * i + half + a * tiles
            keep = low if half == 0 else jnp.logical_not(low)
            mine = jnp.where(keep, turned, 0.0)
            other = pltpu.roll(mine, 4 if half == 0 else LANES - 4, 1)
            afeat[half * 3 * tiles + t] = mine.astype(jnp.bfloat16)
            afeat[(1 - half) * 3 * tiles + t] = other.astype(jnp.bfloat16)
        drain(accs, past)
        whole = jnp.concatenate(
            [turned.astype(jnp.bfloat16), jnp.zeros((tile_len, 256 - LANES), jnp.bfloat16)], axis=1
        )
        for p in range(tile_len // PIECE):
            pltpu.matmul_acc_lhs(accs[p], whole[p * PIECE : (p + 1) * PIECE])

    def drain(accs, past):
        for p in range(tile_len // PIECE):
            value = pltpu.matmul_pop(accs[p])
            for half in range(2):
                wcol[past[half], p * PIECE : (p + 1) * PIECE, :] = value[
                    :, half * LANES : (half + 1) * LANES
                ]

    def enlist(t, a):
        spot = t + a * tiles
        high_bits = lax.shift_left(spot, 16)
        for r in range(used):
            code = codes[r, spot]
            items[lax.shift_right_logical(code, 16)] = high_bits + jnp.bitwise_and(code, 65535)

    def prepare(a, accs):
        bring((0, R + 1, R + 2)[a]).wait()

        def pair_of(i, past):
            enlist(2 * i, a)
            enlist(2 * i + 1, a)
            own_pair(i, a, accs, past)
            return 2 * i + a * tiles, 2 * i + 1 + a * tiles

        nowhere = jnp.int32(3 * tiles)
        drain(accs, lax.fori_loop(0, tiles // 2, pair_of, (nowhere, nowhere), unroll=4))

    hands[...] = jnp.zeros_like(hands)

    def clear(t, carry):
        gacc[t] = jnp.zeros((tile_len, LANES), jnp.float32)
        return carry

    lax.fori_loop(0, 3 * tiles, clear, 0)
    decode.wait()

    def outset(*accs):
        for ref in accs:
            pltpu.matmul_pop(ref)
        line = lax.broadcasted_iota(jnp.int32, (32, 256), 0)
        spread = lax.broadcasted_iota(jnp.int32, (32, 256), 1)
        wanted = jnp.bitwise_and(line, 7) == jnp.where(spread < LANES, 3, 7)
        wanted = jnp.logical_and(wanted, line >= 8)
        rhs = jnp.concatenate(
            [
                jnp.zeros((64, 256), jnp.bfloat16),
                jnp.where(wanted, 1.0, 0.0).astype(jnp.bfloat16),
                jnp.zeros((160, 256), jnp.bfloat16),
            ],
            axis=0,
        )
        pltpu.matmul_push_rhs(rhs, staging_register=0, mxu_index=0)
        pltpu.matmul_acc_lhs(
            accs[0], jnp.zeros((PIECE, 256), jnp.bfloat16), load_staged_rhs=0
        )
        prepare(0, accs)
        for side, there in near:
            pl.when(there)(functools.partial(prepare, side + 1, accs))
        rest_of(*accs)

    def rest_of(*accs):
        for k in range(1, R + 1):
            bring(k).wait()

        def ext_pair(i, k):
            at = k * (tiles // 2) + i
            block = block_of(k, i)
            low, high, s = halves(block, 3)
            filled = s > 0.0
            place = block * scale + (base + jnp.where(part == 0, k * quarter, 0.0))
            place = jnp.where(jnp.logical_and(part < 3, filled), place, 0.0)
            s = jnp.where(filled, s, 1.0)
            s2 = s * s
            square = place * place
            pairsum = square + pltpu.roll(square, 1, 0)
            total = pairsum + pltpu.roll(pairsum, 2, 0)
            tail = jnp.where(filled, s2 * (total + 0.0001 / (R * R)), 128.0)
            full = jnp.where(part == 3, s2, -2.0 * s2 * place)
            one, two, three = splits(full)
            first, second, third = splits(tail)
            stack = jnp.concatenate(
                [one, two, one, two, three, one, first, second, third, jnp.zeros_like(one)],
                axis=0,
            )
            bfeat[at] = stack.astype(jnp.bfloat16)
            for half, root in enumerate((low, high)):
                root = jnp.where(root > 0.0, root, 1.0)
                brow[at * 2 + half, :8] = 2.0 * root
                brow[at * 2 + half, 8:] = 4.0 * root * root * root

        def ext_pairs(i, carry):
            for k in range(R + 1):
                ext_pair(i, k)
            return carry

        lax.fori_loop(0, tiles // 2, ext_pairs, 0, unroll=2)
        nothing = ((3 * tiles) << 16) + slots
        for c in range(6):
            items[codes[used, c]] = nothing
        ends = [codes[used + 1, c] for c in range(classes + 1)]
        body(ends, *accs)

    def body(ends, *accs):
        pieces = tile_len // PIECE

        def fields(m):
            packed = items[m]
            at = jnp.bitwise_and(packed, 65535)
            return at, lax.shift_right_logical(packed, 16)

        def push(m, q):
            at, _ = fields(m)
            rhs = jnp.concatenate(
                [
                    bfeat[lax.shift_right_logical(at, 1)],
                    jnp.zeros((256 - 80, tile_len), jnp.bfloat16),
                ],
                axis=0,
            )
            pltpu.matmul_push_rhs(rhs, staging_register=0, mxu_index=q)

        def feed(which, q, p):
            lhs = afeat[which, p * PIECE : (p + 1) * PIECE]
            lhs = jnp.concatenate([lhs, jnp.zeros((PIECE, 256 - LANES), jnp.bfloat16)], axis=1)
            pltpu.matmul_acc_lhs(
                accs[q * pieces + p], lhs, load_staged_rhs=0 if p == 0 else None
            )

        def which_of(m):
            at, t = fields(m)
            return jnp.bitwise_and(at, 1) * (3 * tiles) + t

        def run(j, carry, groups, width):
            now = [fields(2 * j + q) for q in range(2)]
            then = [which_of(2 * j + 2 + q) for q in range(2)]
            rows = [
                [brow[at, r * 8 : r * 8 + 8, h * LANES : (h + 1) * LANES] for r in range(2) for h in range(width)]
                for at, _ in now
            ]
            sums = [[None] * width for _ in now]
            for p in range(pieces if width > 1 else groups * ROWS // PIECE):
                for q, (at, t) in enumerate(now):
                    u = pltpu.matmul_pop(accs[q * pieces + p])
                    feed(then[q], q, p)
                    if p == 0:
                        push(2 * j + 4 + q, q)
                    if p >= groups * ROWS // PIECE:
                        continue
                    for r in range(0, PIECE, 8):
                        here = pl.ds(p * PIECE + r, 8)
                        aw = wcol[t, here, :]
                        total = None
                        for h in range(width):
                            v = u[r : r + 8, h * LANES : (h + 1) * LANES]
                            o = jnp.maximum(rows[q][h] - v * lax.rsqrt(v), 0.0)
                            w = jnp.minimum(o * o * o, rows[q][width + h] - (v * o) * 3.0)
                            total = w if total is None else total + w
                            back = w * aw
                            sums[q][h] = back if sums[q][h] is None else sums[q][h] + back
                        gacc[t, here, :] += total
            for q, (at, t) in enumerate(now):
                for h in range(width):
                    hands[at, :, h * LANES : (h + 1) * LANES] += sums[q][h]
            return carry

        for q in range(2):
            push(q, q)
        for q in range(2):
            for p in range(pieces):
                feed(which_of(q), q, p)
        for q in range(2):
            push(2 + q, q)
        for c in range(classes):
            top = classes // 2
            lax.fori_loop(
                ends[c],
                ends[c + 1],
                functools.partial(run, groups=top - c % top, width=2 - c // top),
                0,
            )
        for q in range(2):
            for p in range(pieces):
                feed(which_of(q), q, p)
        for ref in accs:
            pltpu.matmul_pop(ref)

    pl.run_scoped(
        outset,
        *[pltpu.ACC(q)((PIECE, 256), jnp.float32) for q in range(2) for _ in range(tile_len // PIECE)],
    )
    lane = lax.broadcasted_iota(jnp.int32, (tile_len, LANES), 1)

    def finish(a):
        columns = jnp.zeros((tile_len, LANES), jnp.float32)
        for t in range(tiles):
            value = jnp.sum(gacc[a * tiles + t], axis=1, keepdims=True)
            columns = jnp.where(lane == t, value, columns)
        gained_ref[a] = jnp.transpose(columns, (1, 0))[:tiles]

    finish(0)
    for side, there in near:
        pl.when(there)(functools.partial(finish, side + 1))
    handed_ref[...] = jnp.sum(hands[tiles:slots], axis=1).reshape(handed_ref.shape)


def pairs(codes, ext, walls):
    tiles = ext.shape[2] // 4
    tile_len = ext.shape[1] * LANES
    hbm = pl.BlockSpec(memory_space=pl.ANY)
    vmem = pl.BlockSpec(memory_space=pltpu.VMEM)
    slots = (R + 1) * tiles
    entries = 3 * slots * NB
    return pl.pallas_call(
        functools.partial(pair_kernel, walls),
        out_shape=(
            jax.ShapeDtypeStruct((3, tiles, tile_len), jnp.float32),
            jax.ShapeDtypeStruct((R, tiles, tile_len), jnp.float32),
        ),
        in_specs=[hbm, hbm],
        out_specs=(vmem, vmem),
        scratch_shapes=[
            pltpu.VMEM((6 * tiles, tile_len, LANES), jnp.bfloat16),
            pltpu.VMEM((3 * tiles + 1, tile_len, LANES), jnp.float32),
            pltpu.VMEM((slots // 2 + 1, 80, tile_len), jnp.bfloat16),
            pltpu.VMEM((slots + 1, 16, tile_len), jnp.float32),
            pltpu.VMEM((3 * tiles + 1, tile_len, LANES), jnp.float32),
            pltpu.VMEM((slots + 1, 8, tile_len), jnp.float32),
            pltpu.SMEM(codes.shape, jnp.int32),
            pltpu.SMEM((entries + 32,), jnp.int32),
            pltpu.VMEM(ext.shape, jnp.float32),
            pltpu.SemaphoreType.DMA((ext.shape[0],)),
            pltpu.SemaphoreType.DMA,
        ],
    )(codes, ext)


def return_kernel(
    chans,
    walls,
    gained_in,
    handed_in,
    held,
    gained_ref,
    handed_ref,
    send_sem,
    recv_sem,
    local_sem,
):
    chan = lax.axis_index("chan")
    wall = lax.axis_index("wall")
    sides = (wall > 0).astype(jnp.int32) + (wall < walls - 1).astype(jnp.int32)
    pulls = (
        pltpu.make_async_copy(handed_in, handed_ref, local_sem.at[0]),
        pltpu.make_async_copy(gained_in.at[pl.ds(1, 2)], gained_ref, local_sem.at[1]),
    )
    for one in pulls:
        one.start()
    barrier = pltpu.get_barrier_semaphore()
    for k in range(1, R + 1):
        target = (lax.rem(chan + chans - k, chans), wall)
        pl.semaphore_signal(barrier, inc=1, device_id=target, device_id_type=MESH)
    for _, other, there in wall_cases(wall, walls):
        @pl.when(there)
        def _(other=other):
            pl.semaphore_signal(barrier, inc=1, device_id=(chan, other), device_id_type=MESH)
    for one in pulls:
        one.wait()
    pl.semaphore_wait(barrier, R + sides)

    def copy(source, slot, device):
        return pltpu.make_async_remote_copy(
            src_ref=source,
            dst_ref=held.at[slot],
            send_sem=send_sem.at[slot],
            recv_sem=recv_sem.at[slot],
            device_id=device,
            device_id_type=MESH,
        )

    def ahead(k):
        return copy(handed_ref.at[k - 1], k - 1, (lax.rem(chan + k, chans), wall))

    def aside(side, slot, other):
        return copy(gained_ref.at[side], R + slot, (chan, other))

    for k in range(R, 0, -1):
        ahead(k).start()
    for side, other, there in wall_cases(wall, walls):
        @pl.when(there)
        def _(side=side, other=other):
            aside(side, 1 - side, other).start()

    for k in range(1, R + 1):
        ahead(k).wait()
    for side, other, there in wall_cases(wall, walls):
        @pl.when(there)
        def _(side=side, other=other):
            aside(side, side, other).wait_recv()
            aside(side, 1 - side, other).wait_send()


def hand_back(gained, handed, chans, walls):
    _, tiles, tile_len = gained.shape
    hbm = pl.BlockSpec(memory_space=pl.ANY)
    return pl.pallas_call(
        functools.partial(return_kernel, chans, walls),
        out_shape=jax.ShapeDtypeStruct((R + 2, tiles, tile_len), jnp.float32),
        in_specs=[hbm] * 2,
        out_specs=hbm,
        scratch_shapes=[
            pltpu.VMEM((2, tiles, tile_len), jnp.float32),
            pltpu.VMEM(handed.shape, jnp.float32),
            pltpu.SemaphoreType.DMA((R + 2,)),
            pltpu.SemaphoreType.DMA((R + 2,)),
            pltpu.SemaphoreType.DMA((2,)),
        ],
        compiler_params=pltpu.CompilerParams(collective_id=1, has_side_effects=True),
    )(gained, handed)


def total_kernel(walls, scale, gained_ref, held_ref, over_ref, out_ref):
    wall = lax.axis_index("wall")
    _, tiles, tile_len = gained_ref.shape
    parts = tile_len // LANES
    total = gained_ref[0]
    total += jnp.where(wall > 0, held_ref[R], 0.0)
    total += jnp.where(wall < walls - 1, held_ref[R + 1], 0.0)
    handed = held_ref[0]
    for k in range(1, R):
        handed += held_ref[k]
    total = (total * over_ref[0] + handed * over_ref[1]) * scale
    for h in range(parts):
        out_ref[pl.ds(h, tiles, stride=parts), :] = total[:, h * LANES : (h + 1) * LANES]


def add_up(gained, held, over, scale, walls):
    _, tiles, tile_len = gained.shape
    vmem = pl.BlockSpec(memory_space=pltpu.VMEM)
    first = pl.BlockSpec((1, tiles, tile_len), lambda i: (0, 0, 0))
    return pl.pallas_call(
        functools.partial(total_kernel, walls, scale),
        grid=(1,),
        out_shape=jax.ShapeDtypeStruct((tiles * tile_len // LANES, LANES), gained.dtype),
        in_specs=[first, vmem, vmem],
        out_specs=vmem,
    )(gained, held, over)


def on_device(chans, walls, coords, masses, counts, lists):
    tiles = counts.shape[2]
    tile_len = masses.shape[2] // tiles
    scale = 1.0 / (4.0 * math.pi * NB * tile_len)
    lists = jnp.swapaxes(lists.reshape(lists.shape[2:]), 1, 2)
    ext, over, codes = gather(
        coords.reshape(-1, LANES),
        masses.reshape(-1, LANES),
        counts.reshape(-1),
        lists,
        chans,
        walls,
    )
    gained, handed = pairs(codes, ext, walls)
    held = hand_back(gained, handed, chans, walls)
    return add_up(gained, held, over, scale, walls).reshape(1, 1, -1)


def solution(mesh):
    placed = (
        P(None, "chan", "wall", None),
        P("chan", "wall", None),
        P("chan", "wall", None),
        P("chan", "wall", None, None, None),
    )
    body = functools.partial(on_device, mesh.shape["chan"], mesh.shape["wall"])
    return jax.shard_map(
        body, mesh=mesh, in_specs=placed, out_specs=P("chan", "wall", None), check_vma=False
    )
```
